32 devices in a mesh: section: 4 (over y, core), dp: 8 (over z, x).
Axes of the slice: x: 2, y: 2, z: 4, core: 2. Of those that a mesh axis runs over, the one named last changes fastest.
Arguments:
- student_states: bfloat16 [4, 1024, 2048], P('section', 'dp'), may hold values from -6 to 6
- teacher_states: bfloat16 [16, 1024, 7168], P('section', 'dp'), may hold values from -18 to 18
- projector: bfloat16 [4, 2048, 7168], P('section', None, 'dp'), may hold values from -0.125 to 0.125
- layer_map: int32 [4], replicated, may hold values from 0 to 12, as said below
- boundaries: int32 [5], replicated, may hold values from 0 to 13, as said below
- valid_counts: int32 [8], P('dp'), may hold values from 32 to 128, as said below
Outputs:
- student_grads: bfloat16 [4, 1024, 2048], P('section', 'dp')
- projector_grads: bfloat16 [4, 2048, 7168], P('section', None, 'dp')
- layer_losses: float32 [4], P('section')
The draws below stay inside these ranges and needn't reach their ends.
Inputs may be any that keep to these rules, and one draw needn't show every extreme that they name: Section k holds 4 or 3 teacher layers, three sections the smaller number; boundaries[0] is 0 and boundaries[4] is 13. Teacher layer layer_map[l] lies on a section from l - 2 to l + 2; student layers 0 and 3 pair with layers of sections 1 and 2, student layers 1 and 2 with layers of sections 3 and 0. `valid_counts`: the valid tokens stand first in their micro-batch; the last micro-batch is full.
All inputs are finite; a program needn't handle non-finite values.
Results may differ from the reference program's by a relative error of at most 0.015.
Values may be sent and summed in bfloat16 or wider, within the bound.
A program may use at most 128 MiB of HBM per device.

```python
import jax
import jax.numpy as jnp
from jax import lax

DS = 2048
DT = 7168
MB_TOK = 128
TL_DEV = 4
STUDENT_LAYERS = 4
SLOTS = 16
TOKENS = 1024
N_SECTION = 4
N_DP = 8


def section_plan(key):
    base = jax.random.fold_in(key, 17)
    first_key = jax.random.fold_in(base, 1)
    second_key = jax.random.fold_in(base, 2)
    third_key = jax.random.fold_in(base, 3)
    places = jnp.arange(N_SECTION, dtype=jnp.int32)
    shorter = (jax.random.permutation(first_key, N_SECTION) < 3).astype(jnp.int32)
    held = TL_DEV - shorter
    bounds = jnp.concatenate([jnp.zeros((1,), jnp.int32), jnp.cumsum(held).astype(jnp.int32)])
    offsets = jax.random.randint(second_key, (N_SECTION,), -2, 3).astype(jnp.int32)
    owners = jnp.clip(places + offsets, 0, N_SECTION - 1)
    owners = owners.at[1].set(3).at[N_SECTION - 2].set(N_SECTION - 4)
    owners = owners.at[0].set(1).at[N_SECTION - 1].set(N_SECTION - 2)
    within = jax.random.randint(third_key, (N_SECTION,), 0, TL_DEV).astype(jnp.int32) % held[owners]
    mapped = (bounds[owners] + within).astype(jnp.int32)
    return (bounds, mapped)


def draw_layer_map(key, part):
    return section_plan(key)[1]


def draw_boundaries(key, part):
    return section_plan(key)[0]


def draw_valid_counts(key, part):
    places = jnp.arange(N_DP, dtype=jnp.int32)
    lowest = MB_TOK // 4
    rising = lowest + (MB_TOK - lowest) * places // max(N_DP - 1, 1)
    jitter = jax.random.randint(jax.random.fold_in(key, 5), (N_DP,), 0, MB_TOK // 8 + 1).astype(jnp.int32)
    counts = jnp.clip(rising - jitter, lowest, MB_TOK).astype(jnp.int32)
    return counts.at[N_DP - 1].set(MB_TOK)


def levels(key, extent, pieces, least, largest):
    level = 1.0
    for position, shards_of in pieces:
        heights = jax.random.uniform(jax.random.fold_in(jax.random.fold_in(key, 6), position), (shards_of,), jnp.float32, least / len(pieces), largest / len(pieces))
        level = level * jnp.repeat(jnp.exp(heights), extent[position] // shards_of).reshape((-1,) + (1,) * (len(extent) - 1 - position))
    return level


def normal_values(stream_key, shape, scale, most, shards=(), kind=jnp.bfloat16):
    values = jax.random.normal(stream_key, shape, jnp.float32) * scale
    if len(shards) > 0:
        values = levels(stream_key, shape, shards, -0.22, 0.18) * values
    return jnp.clip(values, min=-most, max=most).astype(kind)


def setup_inputs(seed: int = 0) -> dict:
    streams_of = jax.random.split(jax.random.key(seed), 7)
    student_states = normal_values(streams_of[0], (STUDENT_LAYERS, TOKENS, DS), 1.0, 6.0, ((0, 4), (1, 8)))
    teacher_states = normal_values(streams_of[1], (SLOTS, TOKENS, DT), 3.0, 18.0, ((0, 4), (1, 8)))
    projector = normal_values(streams_of[2], (STUDENT_LAYERS, DS, DT), DS ** -0.5, 0.125, ((0, 4), (2, 8)))
    layer_map = draw_layer_map(jax.random.fold_in(streams_of[6], 71), 0)
    boundaries = draw_boundaries(jax.random.fold_in(streams_of[6], 71), 0)
    valid_counts = draw_valid_counts(jax.random.fold_in(streams_of[6], 71), 0)
    return dict(student_states=student_states, teacher_states=teacher_states, projector=projector, layer_map=layer_map, boundaries=boundaries, valid_counts=valid_counts)


loss_scale = 128.0
norm_eps = 1e-06

def reference(student_states, teacher_states, projector, layer_map, boundaries, valid_counts):
    rows = jnp.arange(TOKENS, dtype=jnp.int32)
    limit = valid_counts[rows // MB_TOK]
    valid = (rows % MB_TOK < limit).astype(jnp.float32)[:, None]
    total = jnp.sum(valid_counts).astype(jnp.float32)
    owners = lax.optimization_barrier(jnp.sum((boundaries[None, 1:N_SECTION] <= layer_map[:, None]).astype(jnp.int32), axis=1))
    slots = (owners * TL_DEV + layer_map - boundaries[owners]).astype(jnp.int32)
    group_width = DT // N_DP
    student_list = []
    projector_list = []
    loss_list = []
    for layer in range(STUDENT_LAYERS):
        wide = teacher_states[slots[layer]].astype(jnp.float32)
        target = (wide * lax.rsqrt(lax.optimization_barrier(jnp.mean(wide * wide, axis=1, keepdims=True)) + norm_eps)).astype(jnp.bfloat16)
        projected = jnp.dot(student_states[layer], projector[layer], preferred_element_type=jnp.float32)
        residual = projected - target.astype(jnp.float32)
        loss_list.append(jnp.sum(valid * residual * residual) / (total * DT))
        scaled = (valid * (loss_scale / total) * residual).astype(jnp.bfloat16)
        summed = jnp.zeros((TOKENS, DS), jnp.float32)
        for group in range(N_DP):
            left = scaled[:, group * group_width:(group + 1) * group_width]
            right = projector[layer][:, group * group_width:(group + 1) * group_width]
            piece = jnp.dot(left, right.T, preferred_element_type=jnp.float32).astype(jnp.bfloat16)
            summed = summed + piece.astype(jnp.float32)
        student_list.append(summed.astype(jnp.bfloat16))
        projector_list.append(jnp.dot(student_states[layer].T, scaled, preferred_element_type=jnp.float32).astype(jnp.bfloat16))
    return (jnp.stack(student_list), jnp.stack(projector_list), jnp.stack(loss_list))
```

```python
import functools

import jax
import jax.numpy as jnp
from jax import lax
from jax.experimental import pallas as pl
from jax.experimental.pallas import tpu as pltpu
from jax.sharding import PartitionSpec as P

loss_scale = 128.0
norm_eps = 1e-06
MESH = pl.DeviceIdType.MESH
F32, BF16 = jnp.float32, jnp.bfloat16
CHUNKS = 2
GRAD_TILES = 8


def from_behind(block, axis, distance):
    devices = range(lax.axis_size(axis))
    route = [(i - distance, i) for i in devices if i - distance in devices]
    return lax.ppermute(block, axis, route)


def lookup(table, index):
    places = jnp.arange(table.shape[0], dtype=jnp.int32)
    return jnp.sum(jnp.where(places == index, table, 0))


def relayed(teacher_states, layer_map, boundaries):
    sections = lax.axis_size("section")
    here = lax.axis_index("section")
    held_slots = teacher_states.shape[0]
    inner = boundaries[1:sections]
    owners = jnp.sum((inner[None, :] <= layer_map[:, None]).astype(jnp.int32), axis=1)
    first_layer = lookup(boundaries, here)

    def outgoing(offset):
        destination = here + offset
        inside = (destination >= 0) & (destination < sections)
        wanted = lookup(layer_map, destination)
        owner = lookup(owners, destination)
        place = jnp.clip(wanted - first_layer, 0, held_slots - 1)
        piece = lax.dynamic_index_in_dim(teacher_states, place, 0, keepdims=False)
        return jnp.where(inside & (owner == here), piece, jnp.zeros_like(piece))

    needed = here - lookup(owners, here)
    arrivals = []
    for offset in (-1, 1):
        stacked = jnp.stack([outgoing(offset), outgoing(2 * offset)])
        first_arrived = from_behind(stacked, "section", offset)
        second_arrived = from_behind(first_arrived[1:2], "section", offset)
        arrivals.append((offset, first_arrived[0]))
        arrivals.append((2 * offset, second_arrived[0]))
    hidden = outgoing(0)
    for offset, arrived in arrivals:
        hidden = jnp.where(needed == offset, arrived, hidden)
    return hidden


def send_to(here):
    return 2 - 2 * here + 5 * (here // 2)


def taken_from(here):
    return 1 + 2 * here - 5 * (here // 2)


def pick_kernel(map_ref, bounds_ref, counts_ref, teacher_ref, slab_ref, count_ref, sem):
    here = lax.axis_index("section")
    place = map_ref[send_to(here)] - bounds_ref[here]
    place = jnp.minimum(jnp.maximum(place, 0), teacher_ref.shape[0] - 1)
    copy = pltpu.make_async_copy(teacher_ref.at[place], slab_ref, sem)
    copy.start()
    count_ref[...] = jnp.full(count_ref.shape, counts_ref[0].astype(F32), F32)
    copy.wait()


def pick(teacher_states, layer_map, boundaries, valid_counts):
    smem = pl.BlockSpec(memory_space=pltpu.SMEM)
    vmem = pl.BlockSpec(memory_space=pltpu.VMEM)
    return pl.pallas_call(
        pick_kernel,
        out_shape=(
            jax.ShapeDtypeStruct(teacher_states.shape[1:], BF16),
            jax.ShapeDtypeStruct((8, 128), F32),
        ),
        in_specs=[smem, smem, smem, pl.BlockSpec(memory_space=pl.ANY)],
        out_specs=(vmem, vmem),
        scratch_shapes=[pltpu.SemaphoreType.DMA],
    )(layer_map, boundaries, valid_counts, teacher_states)


def main_kernel(n, direct, s_hbm, slab_hbm, w_hbm, count_ref, sg_ref, pg_hbm, loss_ref,
                slab_ref, weights, stud, normed, tgt, proj, scaled, own, part_a, part_b, got_a, got_b,
                counts, losses, loss_out, pg,
                in_sem, slab_sem, w_sem, ag_send, ag_recv, t_send, t_recv, rs_send, rs_recv,
                c_send, c_recv, l_send, l_recv, pg_sem, passing, p_send, p_recv):
    here = lax.axis_index("section")
    me = lax.axis_index("dp")
    rows, ds_width = s_hbm.shape
    width = weights.shape[1]
    half = rows // CHUNKS
    steps_a, steps_b = n // 2, n - 1 - n // 2
    teacher_width = width * n

    x, z = me % 2, me // 2
    position = z * (1 - x) + (n - 1 - z) * x
    sign = 1 - 2 * (here % 2)

    def at(offset):
        p = (position + sign * offset + 2 * n) % n
        low = 1 - p // (n // 2)
        return low * (2 * p) + (1 - low) * (2 * (n - 1 - p) + 1)

    after, before = at(1), at(-1)

    def block(index):
        return pl.ds(pl.multiple_of(index * rows, rows), rows)

    load_students = pltpu.make_async_copy(s_hbm, stud.at[block(me)], in_sem)
    load_students.start()
    load_slab = pltpu.make_async_copy(slab_hbm, slab_ref, slab_sem)
    load_slab.start()
    barrier = pltpu.get_barrier_semaphore()
    for k in range(1, n):
        pl.semaphore_signal(barrier, inc=1, device_id=(here, (me + k) % n), device_id_type=MESH)
    expected = n - 1
    if direct:
        for k in range(n):
            pl.semaphore_signal(barrier, inc=1, device_id=(send_to(here), (me + k) % n), device_id_type=MESH)
            pl.semaphore_signal(barrier, inc=1, device_id=(taken_from(here), (me + k) % n), device_id_type=MESH)
        expected += 2 * n
    load_weights = pltpu.make_async_copy(w_hbm, weights, w_sem)
    load_weights.start()
    pl.semaphore_wait(barrier, expected)
    load_students.wait()

    pair, line = me % 2, me // 2
    partner = me + 1 - 2 * pair
    lines = n // 2

    def reached(place):
        return (line + lines - place) // lines

    def arrival_of(k):
        value = 0
        for place in range(lines):
            order = []
            for step in range(lines - 1):
                order += [b for b in (place - 1 - step, place + 1 + step) if 0 <= b < lines]
            value = value + order[k] * (reached(place) - reached(place + 1))
        return value

    def piece_of(index, chunk):
        return stud.at[pl.ds(pl.multiple_of(index * rows + chunk * half, half), half)]

    UP, DOWN, ACROSS = 0, 1, 2
    targets_of = (me + 2, me - 2, me + 1 - 2 * pair)

    def ag_copy(way, index, step, chunk):
        return pltpu.make_async_remote_copy(
            src_ref=piece_of(index, chunk), dst_ref=piece_of(index, chunk),
            send_sem=ag_send.at[way, step, chunk], recv_sem=ag_recv.at[index, chunk],
            device_id=(here, targets_of[way]), device_id_type=MESH)

    def ag_arrival(index, chunk):
        return pltpu.make_async_remote_copy(
            src_ref=piece_of(index, chunk), dst_ref=piece_of(index, chunk),
            send_sem=ag_send.at[0, 0, chunk], recv_sem=ag_recv.at[index, chunk],
            device_id=(here, targets_of[2]), device_id_type=MESH)

    ag_steps = (steps_a, steps_b)
    sent = []
    sent_if = []

    def go(copy):
        copy.start()
        sent.append(copy)

    def go_if(condition, copy):
        pl.when(condition)(copy.start)
        sent_if.append((condition, copy))

    can_up, can_down = line < lines - 1, line > 0
    for chunk in range(CHUNKS):
        go_if(can_up, ag_copy(UP, me, 0, chunk))
        go_if(can_down, ag_copy(DOWN, me, 0, chunk))
        go(ag_copy(ACROSS, me, 0, chunk))

    def relay(step):
        below, above = me - 2 - 2 * step, me + 2 + 2 * step
        from_below, from_above = line - 1 - step >= 0, line + 1 + step < lines
        for chunk in range(CHUNKS):
            pl.when(from_below)(ag_arrival(below, chunk).wait_recv)
            go_if(from_below & can_up, ag_copy(UP, below, step + 1, chunk))
            pl.when(from_above)(ag_arrival(above, chunk).wait_recv)
            go_if(from_above & can_down, ag_copy(DOWN, above, step + 1, chunk))
        for chunk in range(CHUNKS):
            go_if(from_below, ag_copy(ACROSS, below, 2 * step + 1, chunk))
        for chunk in range(CHUNKS):
            go_if(from_above, ag_copy(ACROSS, above, 2 * step + 2, chunk))

    def small(source, slots, send_sems, recv_sems, k):
        peer = (me + k) % n
        return pltpu.make_async_remote_copy(
            src_ref=source, dst_ref=slots.at[me], send_sem=send_sems.at[k], recv_sem=recv_sems.at[me],
            device_id=(here, peer), device_id_type=MESH)

    def small_arrival(slots, send_sems, recv_sems, k):
        peer = (me + k) % n
        return pltpu.make_async_remote_copy(
            src_ref=slots.at[peer], dst_ref=slots.at[peer], send_sem=send_sems.at[k],
            recv_sem=recv_sems.at[peer], device_id=(here, peer), device_id_type=MESH)

    for k in range(1, n):
        go(small(count_ref, counts, c_send, c_recv, k))
    counts[me] = count_ref[...]

    load_slab.wait()
    squares = jnp.zeros((rows, 1), F32)
    for g in range(n):
        h = slab_ref[:, g * width:(g + 1) * width].astype(F32)
        squares += jnp.sum(h * h, axis=1, keepdims=True)
    inverse = lax.rsqrt(squares / teacher_width + norm_eps)
    for g in range(n):
        h = slab_ref[:, g * width:(g + 1) * width].astype(F32)
        normed[g] = (h * inverse).astype(BF16)
    taker = send_to(here) if direct else here

    def target_copy(source, owner, g):
        return pltpu.make_async_remote_copy(
            src_ref=source, dst_ref=tgt.at[block(owner)], send_sem=t_send.at[owner, g], recv_sem=t_recv.at[owner],
            device_id=(taker, g), device_id_type=MESH)

    def crossing(k):
        g = 2 * ((line + k) % lines) + 1 - pair
        return pltpu.make_async_remote_copy(
            src_ref=normed.at[g], dst_ref=passing.at[k], send_sem=p_send.at[k], recv_sem=p_recv.at[k],
            device_id=(here, partner), device_id_type=MESH)

    def own_target(k):
        g = 2 * ((line + k) % lines) + pair
        return target_copy(normed.at[g], me, g)

    def passed_target(k):
        g = 2 * ((line + k) % lines) + pair
        return target_copy(passing.at[k], partner, g)

    def target_arrival(index):
        return pltpu.make_async_remote_copy(
            src_ref=tgt.at[block(index)], dst_ref=tgt.at[block(index)], send_sem=t_send.at[0, index],
            recv_sem=t_recv.at[index], device_id=(taker, index), device_id_type=MESH)

    if not direct:
        tgt[block(me), :] = normed[me]
    for k in range(1, lines):
        go(crossing(k))
    go(target_copy(normed.at[partner], me, partner))
    if direct:
        go(own_target(0))

    def project(index):
        proj[block(index), :] = jnp.dot(stud[block(index), :], weights[...], preferred_element_type=F32)

    row = lax.broadcasted_iota(jnp.int32, (rows, 1), 0).astype(F32)
    losses[me] = jnp.zeros(losses.shape[1:], F32)

    def total():
        value = counts[0][0:1, :]
        for b in range(1, n):
            value = value + counts[b][0:1, :]
        return value

    def residual(offset):
        index = at(offset)
        if direct or offset != 0:
            target_arrival(index).wait_recv()
        left = proj[block(index), :] - tgt[block(index), :].astype(F32)
        valid = jnp.where(row < counts[index][0:1, 0:1], 1.0, 0.0)
        kept = valid * left
        line = jnp.sum(kept * left, axis=0, keepdims=True)
        losses[me] += jnp.broadcast_to(line, losses.shape[1:])
        scaled[block(index), :] = (loss_scale / total()[:, 0:1] * kept).astype(BF16)

    def share(offset, into):
        own[into] = lax.dot_general(
            scaled[block(at(offset)), :], weights[...], (((1,), (1,)), ((), ())), preferred_element_type=F32)

    def rs_copy(direction, step, chunk):
        parts, gots = (part_a, got_a) if direction == 0 else (part_b, got_b)
        piece = pl.ds(chunk * half, half)
        return pltpu.make_async_remote_copy(
            src_ref=parts.at[step, piece], dst_ref=gots.at[step, piece],
            send_sem=rs_send.at[direction, step, chunk], recv_sem=rs_recv.at[direction, step, chunk],
            device_id=(here, after if direction == 0 else before), device_id_type=MESH)

    def grad_tile(tile):
        size = ds_width // GRAD_TILES
        left = stud[:, tile * size:(tile + 1) * size]
        pg[tile * size:(tile + 1) * size, :] = lax.dot_general(
            left, scaled[...], (((0,), (0,)), ((), ())), preferred_element_type=F32).astype(BF16)
        piece = pl.ds(tile * size, size)
        go_local = pltpu.make_async_copy(pg.at[piece], pg_hbm.at[piece], pg_sem.at[tile])
        go_local.start()
        return go_local

    def advance(step, directions):
        for chunk in range(CHUNKS):
            piece = slice(chunk * half, (chunk + 1) * half)
            for direction in directions:
                if step >= ag_steps[direction]:
                    continue
                parts, gots = (part_a, got_a) if direction == 0 else (part_b, got_b)
                value = own[direction, piece, :]
                if step > 0:
                    rs_copy(direction, step - 1, chunk).wait_recv()
                    value = value + gots[step - 1, piece, :].astype(F32)
                parts[step, piece, :] = value.astype(BF16)
                go(rs_copy(direction, step, chunk))

    def prepare(step, direction):
        if step < ag_steps[direction]:
            offset = steps_a - step if direction == 0 else step - steps_b
            residual(offset)
            share(offset, direction)

    def project_across(source):
        index = 2 * source + 1 - pair
        for chunk in range(CHUNKS):
            ag_arrival(index, chunk).wait_recv()
        project(index)

    load_weights.wait()
    project(me)
    for step in range(lines - 1):
        relay(step)
        if step == min(1, lines - 2):
            for k in range(lines - 1, 0, -1):
                go(own_target(k))
        project(2 * arrival_of(step) + pair)
        if step == 0:
            for k in range(1, n):
                small_arrival(counts, c_send, c_recv, k).wait_recv()
            project_across(line)
        if step == min(1, lines - 2):
            for k in range(1, lines):
                crossing(k).wait_recv()
                go(passed_target(k))
    for step in range(lines - 1):
        project_across(arrival_of(step))

    prepare(0, 1)
    advance(0, (1,))
    prepare(0, 0)
    advance(0, (0,))
    for step in range(1, steps_a):
        prepare(step, 1)
        prepare(step, 0)
        if step == steps_a - 1:
            residual(0)
            share(0, 1)
        advance(step, (1, 0))

    line = losses[me][0:1, :]
    folded = jnp.sum(line, axis=1, keepdims=True)
    loss_out[me] = jnp.broadcast_to(folded, loss_out.shape[1:])
    written = [grad_tile(0)]
    for k in range(1, n):
        go(small(loss_out.at[me], loss_out, l_send, l_recv, k))
    for tile in range(1, GRAD_TILES):
        written.append(grad_tile(tile))

    for k in range(1, n):
        small_arrival(loss_out, l_send, l_recv, k).wait_recv()
    whole = loss_out[0][0:1, :]
    count = total()
    for b in range(1, n):
        whole = whole + loss_out[b][0:1, :]
    loss_ref[...] = jnp.broadcast_to(whole / (count * teacher_width), loss_ref.shape)

    for chunk in range(CHUNKS):
        piece = slice(chunk * half, (chunk + 1) * half)
        value = own[1, piece, :]
        rs_copy(0, steps_a - 1, chunk).wait_recv()
        value = value + got_a[steps_a - 1, piece, :].astype(F32)
        if steps_b > 0:
            rs_copy(1, steps_b - 1, chunk).wait_recv()
            value = value + got_b[steps_b - 1, piece, :].astype(F32)
        sg_ref[piece, :] = value.astype(BF16)
    for copy in written:
        copy.wait()
    for copy in sent:
        copy.wait_send()
    for condition, copy in sent_if:
        pl.when(condition)(copy.wait_send)


def per_device(student_states, teacher_states, projector, layer_map, boundaries, valid_counts):
    n = lax.axis_size("dp")
    rows, ds_width = student_states.shape[1:]
    width = projector.shape[2]
    direct = lax.axis_size("section") == 4
    if direct:
        slab, count = pick(teacher_states, layer_map, boundaries, valid_counts)
    else:
        slab = relayed(teacher_states, layer_map, boundaries)
        count = jnp.full((8, 128), valid_counts[0].astype(F32), F32)
    steps_a, steps_b = n // 2, n - 1 - n // 2
    vmem = pl.BlockSpec(memory_space=pltpu.VMEM)
    anywhere = pl.BlockSpec(memory_space=pl.ANY)
    dma = pltpu.SemaphoreType.DMA
    student_grad, projector_grad, loss = pl.pallas_call(
        functools.partial(main_kernel, n, direct),
        out_shape=(
            jax.ShapeDtypeStruct((rows, ds_width), BF16),
            jax.ShapeDtypeStruct((ds_width, width), BF16),
            jax.ShapeDtypeStruct((8, 128), F32),
        ),
        in_specs=[anywhere, anywhere, anywhere, vmem],
        out_specs=(vmem, anywhere, vmem),
        scratch_shapes=[
            pltpu.VMEM((rows, n * width), BF16),
            pltpu.VMEM((ds_width, width), BF16),
            pltpu.VMEM((n * rows, ds_width), BF16),
            pltpu.VMEM((n, rows, width), BF16),
            pltpu.VMEM((n * rows, width), BF16),
            pltpu.VMEM((n * rows, width), F32),
            pltpu.VMEM((n * rows, width), BF16),
            pltpu.VMEM((2, rows, ds_width), F32),
            pltpu.VMEM((steps_a, rows, ds_width), BF16),
            pltpu.VMEM((max(steps_b, 1), rows, ds_width), BF16),
            pltpu.VMEM((steps_a, rows, ds_width), BF16),
            pltpu.VMEM((max(steps_b, 1), rows, ds_width), BF16),
            pltpu.VMEM((n, 8, 128), F32),
            pltpu.VMEM((n, 8, width), F32),
            pltpu.VMEM((n, 8, 128), F32),
            pltpu.VMEM((ds_width, width), BF16),
            dma,
            dma,
            dma,
            dma((3, n, CHUNKS)),
            dma((n, CHUNKS)),
            dma((n, n)),
            dma((n,)),
            dma((2, steps_a, CHUNKS)),
            dma((2, steps_a, CHUNKS)),
            dma((n,)),
            dma((n,)),
            dma((n,)),
            dma((n,)),
            dma((GRAD_TILES,)),
            pltpu.VMEM((n // 2, rows, width), BF16),
            dma((n // 2,)),
            dma((n // 2,)),
        ],
        compiler_params=pltpu.CompilerParams(
            collective_id=0, has_side_effects=True, vmem_limit_bytes=56 * 1024 * 1024
        ),
    )(student_states[0], slab, projector[0], count)
    return student_grad[None], projector_grad[None], loss[0, 0:1]


def solution(mesh):
    in_specs = (
        P("section", "dp", None),
        P("section", "dp", None),
        P("section", None, "dp"),
        P(),
        P(),
        P("dp"),
    )
    out_specs = (P("section", "dp", None), P("section", None, "dp"), P("section"))
    return jax.shard_map(
        per_device, mesh=mesh, in_specs=in_specs, out_specs=out_specs, check_vma=False
    )
```

```python
import functools

import jax
import jax.numpy as jnp
from jax import lax
from jax.experimental import pallas as pl
from jax.experimental.pallas import tpu as pltpu
from jax.sharding import PartitionSpec as P

loss_scale = 128.0
norm_eps = 1e-06
MESH = pl.DeviceIdType.MESH
F32, BF16 = jnp.float32, jnp.bfloat16
CHUNKS = 2
GRAD_TILES = 8


def from_behind(block, axis, distance):
    devices = range(lax.axis_size(axis))
    route = [(i - distance, i) for i in devices if i - distance in devices]
    return lax.ppermute(block, axis, route)


def lookup(table, index):
    places = jnp.arange(table.shape[0], dtype=jnp.int32)
    return jnp.sum(jnp.where(places == index, table, 0))


def relayed(teacher_states, layer_map, boundaries):
    sections = lax.axis_size("section")
    here = lax.axis_index("section")
    held_slots = teacher_states.shape[0]
    inner = boundaries[1:sections]
    owners = jnp.sum((inner[None, :] <= layer_map[:, None]).astype(jnp.int32), axis=1)
    first_layer = lookup(boundaries, here)

    def outgoing(offset):
        destination = here + offset
        inside = (destination >= 0) & (destination < sections)
        wanted = lookup(layer_map, destination)
        owner = lookup(owners, destination)
        place = jnp.clip(wanted - first_layer, 0, held_slots - 1)
        piece = lax.dynamic_index_in_dim(teacher_states, place, 0, keepdims=False)
        return jnp.where(inside & (owner == here), piece, jnp.zeros_like(piece))

    needed = here - lookup(owners, here)
    arrivals = []
    for offset in (-1, 1):
        stacked = jnp.stack([outgoing(offset), outgoing(2 * offset)])
        first_arrived = from_behind(stacked, "section", offset)
        second_arrived = from_behind(first_arrived[1:2], "section", offset)
        arrivals.append((offset, first_arrived[0]))
        arrivals.append((2 * offset, second_arrived[0]))
    hidden = outgoing(0)
    for offset, arrived in arrivals:
        hidden = jnp.where(needed == offset, arrived, hidden)
    return hidden


def send_to(here):
    return 2 - 2 * here + 5 * (here // 2)


def taken_from(here):
    return 1 + 2 * here - 5 * (here // 2)


def main_kernel(n, direct, map_ref, bounds_ref, counts_ref, s_hbm, t_hbm, w_hbm, sg_ref, pg, loss_ref,
                teacher, count_ref, weights, stud, normed, tgt, proj, scaled, own, part_a, part_b, got_a, got_b,
                counts, losses, loss_out,
                in_sem, slab_sem, w_sem, ag_send, ag_recv, t_send, t_recv, rs_send, rs_recv,
                c_send, c_recv, l_send, l_recv, passing, p_send, p_recv):
    here = lax.axis_index("section")
    me = lax.axis_index("dp")
    rows, ds_width = s_hbm.shape
    width = weights.shape[1]
    half = rows // CHUNKS
    steps_a, steps_b = n // 2, n - 1 - n // 2
    teacher_width = width * n

    x, z = me % 2, me // 2
    position = z * (1 - x) + (n - 1 - z) * x
    sign = 1 - 2 * (here % 2)

    def at(offset):
        p = (position + sign * offset + 2 * n) % n
        low = 1 - p // (n // 2)
        return low * (2 * p) + (1 - low) * (2 * (n - 1 - p) + 1)

    after, before = at(1), at(-1)

    def block(index):
        return pl.ds(pl.multiple_of(index * rows, rows), rows)

    load_students = pltpu.make_async_copy(s_hbm, stud.at[block(me)], in_sem)
    load_students.start()
    held = teacher.shape[0]
    load_teacher = [
        pltpu.make_async_copy(t_hbm.at[slot], teacher.at[slot], slab_sem.at[slot]) for slot in range(held)
    ]
    barrier = pltpu.get_barrier_semaphore()
    for k in range(1, n):
        pl.semaphore_signal(barrier, inc=1, device_id=(here, (me + k) % n), device_id_type=MESH)
    expected = n - 1
    if direct:
        for k in range(n):
            pl.semaphore_signal(barrier, inc=1, device_id=(send_to(here), (me + k) % n), device_id_type=MESH)
            pl.semaphore_signal(barrier, inc=1, device_id=(taken_from(here), (me + k) % n), device_id_type=MESH)
        expected += 2 * n
    load_weights = pltpu.make_async_copy(w_hbm, weights, w_sem)
    for copy in load_teacher:
        copy.start()
    load_weights.start()
    count_ref[...] = jnp.full(count_ref.shape, counts_ref[0].astype(F32), F32)
    pl.semaphore_wait(barrier, expected)
    load_students.wait()

    pair, line = me % 2, me // 2
    partner = me + 1 - 2 * pair
    lines = n // 2

    def reached(place):
        return (line + lines - place) // lines

    def arrival_of(k):
        value = 0
        for place in range(lines):
            order = []
            for step in range(lines - 1):
                order += [b for b in (place - 1 - step, place + 1 + step) if 0 <= b < lines]
            value = value + order[k] * (reached(place) - reached(place + 1))
        return value

    def piece_of(index, chunk):
        return stud.at[pl.ds(pl.multiple_of(index * rows + chunk * half, half), half)]

    UP, DOWN, ACROSS = 0, 1, 2
    targets_of = (me + 2, me - 2, me + 1 - 2 * pair)

    def ag_copy(way, index, step, chunk):
        return pltpu.make_async_remote_copy(
            src_ref=piece_of(index, chunk), dst_ref=piece_of(index, chunk),
            send_sem=ag_send.at[way, step, chunk], recv_sem=ag_recv.at[index, chunk],
            device_id=(here, targets_of[way]), device_id_type=MESH)

    def ag_arrival(index, chunk):
        return pltpu.make_async_remote_copy(
            src_ref=piece_of(index, chunk), dst_ref=piece_of(index, chunk),
            send_sem=ag_send.at[0, 0, chunk], recv_sem=ag_recv.at[index, chunk],
            device_id=(here, targets_of[2]), device_id_type=MESH)

    ag_steps = (steps_a, steps_b)
    sent = []
    sent_if = []

    def go(copy):
        copy.start()
        sent.append(copy)

    def go_if(condition, copy):
        pl.when(condition)(copy.start)
        sent_if.append((condition, copy))

    can_up, can_down = line < lines - 1, line > 0
    for chunk in range(CHUNKS):
        go_if(can_up, ag_copy(UP, me, 0, chunk))
        go_if(can_down, ag_copy(DOWN, me, 0, chunk))
        go(ag_copy(ACROSS, me, 0, chunk))

    def relay(step):
        below, above = me - 2 - 2 * step, me + 2 + 2 * step
        from_below, from_above = line - 1 - step >= 0, line + 1 + step < lines
        for chunk in range(CHUNKS):
            pl.when(from_below)(ag_arrival(below, chunk).wait_recv)
            go_if(from_below & can_up, ag_copy(UP, below, step + 1, chunk))
            pl.when(from_above)(ag_arrival(above, chunk).wait_recv)
            go_if(from_above & can_down, ag_copy(DOWN, above, step + 1, chunk))
        for chunk in range(CHUNKS):
            go_if(from_below, ag_copy(ACROSS, below, 2 * step + 1, chunk))
        for chunk in range(CHUNKS):
            go_if(from_above, ag_copy(ACROSS, above, 2 * step + 2, chunk))

    def small(source, slots, send_sems, recv_sems, k):
        peer = (me + k) % n
        return pltpu.make_async_remote_copy(
            src_ref=source, dst_ref=slots.at[me], send_sem=send_sems.at[k], recv_sem=recv_sems.at[me],
            device_id=(here, peer), device_id_type=MESH)

    def small_arrival(slots, send_sems, recv_sems, k):
        peer = (me + k) % n
        return pltpu.make_async_remote_copy(
            src_ref=slots.at[peer], dst_ref=slots.at[peer], send_sem=send_sems.at[k],
            recv_sem=recv_sems.at[peer], device_id=(here, peer), device_id_type=MESH)

    for k in range(1, n):
        go(small(count_ref, counts, c_send, c_recv, k))
    counts[me] = count_ref[...]

    for copy in load_teacher:
        copy.wait()
    place = 0
    if direct:
        place = jnp.clip(map_ref[send_to(here)] - bounds_ref[here], 0, held - 1)
    squares = jnp.zeros((rows, 1), F32)
    for g in range(n):
        h = teacher[place, :, g * width:(g + 1) * width].astype(F32)
        squares += jnp.sum(h * h, axis=1, keepdims=True)
    inverse = lax.rsqrt(squares / teacher_width + norm_eps)
    for g in range(n):
        h = teacher[place, :, g * width:(g + 1) * width].astype(F32)
        normed[g] = (h * inverse).astype(BF16)
    taker = send_to(here) if direct else here

    def target_copy(source, owner, g):
        return pltpu.make_async_remote_copy(
            src_ref=source, dst_ref=tgt.at[block(owner)], send_sem=t_send.at[owner, g], recv_sem=t_recv.at[owner],
            device_id=(taker, g), device_id_type=MESH)

    def crossing(k):
        g = 2 * ((line + k) % lines) + 1 - pair
        return pltpu.make_async_remote_copy(
            src_ref=normed.at[g], dst_ref=passing.at[k], send_sem=p_send.at[k], recv_sem=p_recv.at[k],
            device_id=(here, partner), device_id_type=MESH)

    def own_target(k):
        g = 2 * ((line + k) % lines) + pair
        return target_copy(normed.at[g], me, g)

    def passed_target(k):
        g = 2 * ((line + k) % lines) + pair
        return target_copy(passing.at[k], partner, g)

    def target_arrival(index):
        return pltpu.make_async_remote_copy(
            src_ref=tgt.at[block(index)], dst_ref=tgt.at[block(index)], send_sem=t_send.at[0, index],
            recv_sem=t_recv.at[index], device_id=(taker, index), device_id_type=MESH)

    if not direct:
        tgt[block(me), :] = normed[me]
    for k in range(1, lines):
        go(crossing(k))
    go(target_copy(normed.at[partner], me, partner))
    if direct:
        go(own_target(0))

    def project(index):
        proj[block(index), :] = jnp.dot(stud[block(index), :], weights[...], preferred_element_type=F32)

    row = lax.broadcasted_iota(jnp.int32, (rows, 1), 0).astype(F32)
    losses[me] = jnp.zeros(losses.shape[1:], F32)

    def total():
        value = counts[0][0:1, :]
        for b in range(1, n):
            value = value + counts[b][0:1, :]
        return value

    def residual(offset):
        index = at(offset)
        if direct or offset != 0:
            target_arrival(index).wait_recv()
        left = proj[block(index), :] - tgt[block(index), :].astype(F32)
        valid = jnp.where(row < counts[index][0:1, 0:1], 1.0, 0.0)
        kept = valid * left
        line = jnp.sum(kept * left, axis=0, keepdims=True)
        losses[me] += jnp.broadcast_to(line, losses.shape[1:])
        scaled[block(index), :] = (loss_scale / total()[:, 0:1] * kept).astype(BF16)

    def share(offset, into):
        own[into] = lax.dot_general(
            scaled[block(at(offset)), :], weights[...], (((1,), (1,)), ((), ())), preferred_element_type=F32)

    def rs_copy(direction, step, chunk):
        parts, gots = (part_a, got_a) if direction == 0 else (part_b, got_b)
        piece = pl.ds(chunk * half, half)
        return pltpu.make_async_remote_copy(
            src_ref=parts.at[step, piece], dst_ref=gots.at[step, piece],
            send_sem=rs_send.at[direction, step, chunk], recv_sem=rs_recv.at[direction, step, chunk],
            device_id=(here, after if direction == 0 else before), device_id_type=MESH)

    def grad_tile(tile):
        size = ds_width // GRAD_TILES
        left = stud[:, tile * size:(tile + 1) * size]
        pg[tile * size:(tile + 1) * size, :] = lax.dot_general(
            left, scaled[...], (((0,), (0,)), ((), ())), preferred_element_type=F32).astype(BF16)

    def advance(step, directions):
        for chunk in range(CHUNKS):
            piece = slice(chunk * half, (chunk + 1) * half)
            for direction in directions:
                if step >= ag_steps[direction]:
                    continue
                parts, gots = (part_a, got_a) if direction == 0 else (part_b, got_b)
                value = own[direction, piece, :]
                if step > 0:
                    rs_copy(direction, step - 1, chunk).wait_recv()
                    value = value + gots[step - 1, piece, :].astype(F32)
                parts[step, piece, :] = value.astype(BF16)
                go(rs_copy(direction, step, chunk))

    def prepare(step, direction):
        if step < ag_steps[direction]:
            offset = steps_a - step if direction == 0 else step - steps_b
            residual(offset)
            share(offset, direction)

    def project_across(source):
        index = 2 * source + 1 - pair
        for chunk in range(CHUNKS):
            ag_arrival(index, chunk).wait_recv()
        project(index)

    load_weights.wait()
    project(me)
    for step in range(lines - 1):
        relay(step)
        if step == min(1, lines - 2):
            for k in range(lines - 1, 0, -1):
                go(own_target(k))
        project(2 * arrival_of(step) + pair)
        if step == 0:
            for k in range(1, n):
                small_arrival(counts, c_send, c_recv, k).wait_recv()
            project_across(line)
        if step == min(1, lines - 2):
            for k in range(1, lines):
                crossing(k).wait_recv()
                go(passed_target(k))
    for step in range(lines - 1):
        project_across(arrival_of(step))

    prepare(0, 1)
    advance(0, (1,))
    prepare(0, 0)
    advance(0, (0,))
    for step in range(1, steps_a):
        prepare(step, 1)
        prepare(step, 0)
        if step == steps_a - 1:
            residual(0)
            share(0, 1)
        advance(step, (1, 0))

    line = losses[me][0:1, :]
    folded = jnp.sum(line, axis=1, keepdims=True)
    loss_out[me] = jnp.broadcast_to(folded, loss_out.shape[1:])
    grad_tile(0)
    for k in range(1, n):
        go(small(loss_out.at[me], loss_out, l_send, l_recv, k))
    for tile in range(1, GRAD_TILES):
        grad_tile(tile)

    for k in range(1, n):
        small_arrival(loss_out, l_send, l_recv, k).wait_recv()
    whole = loss_out[0][0:1, :]
    count = total()
    for b in range(1, n):
        whole = whole + loss_out[b][0:1, :]
    loss_ref[...] = jnp.broadcast_to(whole / (count * teacher_width), loss_ref.shape)

    for chunk in range(CHUNKS):
        piece = slice(chunk * half, (chunk + 1) * half)
        value = own[1, piece, :]
        rs_copy(0, steps_a - 1, chunk).wait_recv()
        value = value + got_a[steps_a - 1, piece, :].astype(F32)
        if steps_b > 0:
            rs_copy(1, steps_b - 1, chunk).wait_recv()
            value = value + got_b[steps_b - 1, piece, :].astype(F32)
        sg_ref[piece, :] = value.astype(BF16)
    for copy in sent:
        copy.wait_send()
    for condition, copy in sent_if:
        pl.when(condition)(copy.wait_send)


def per_device(student_states, teacher_states, projector, layer_map, boundaries, valid_counts):
    n = lax.axis_size("dp")
    rows, ds_width = student_states.shape[1:]
    width = projector.shape[2]
    direct = lax.axis_size("section") == 4
    teacher = teacher_states if direct else relayed(teacher_states, layer_map, boundaries)[None]
    steps_a, steps_b = n // 2, n - 1 - n // 2
    smem = pl.BlockSpec(memory_space=pltpu.SMEM)
    vmem = pl.BlockSpec(memory_space=pltpu.VMEM)
    anywhere = pl.BlockSpec(memory_space=pl.ANY)
    dma = pltpu.SemaphoreType.DMA
    student_grad, projector_grad, loss = pl.pallas_call(
        functools.partial(main_kernel, n, direct),
        out_shape=(
            pltpu.VMEM((rows, ds_width), BF16),
            pltpu.VMEM((ds_width, width), BF16),
            pltpu.VMEM((8, 128), F32),
        ),
        in_specs=[smem, smem, smem, anywhere, anywhere, anywhere],
        out_specs=(vmem, vmem, vmem),
        scratch_shapes=[
            pltpu.VMEM(teacher.shape, BF16),
            pltpu.VMEM((8, 128), F32),
            pltpu.VMEM((ds_width, width), BF16),
            pltpu.VMEM((n * rows, ds_width), BF16),
            pltpu.VMEM((n, rows, width), BF16),
            pltpu.VMEM((n * rows, width), BF16),
            pltpu.VMEM((n * rows, width), F32),
            pltpu.VMEM((n * rows, width), BF16),
            pltpu.VMEM((2, rows, ds_width), F32),
            pltpu.VMEM((steps_a, rows, ds_width), BF16),
            pltpu.VMEM((max(steps_b, 1), rows, ds_width), BF16),
            pltpu.VMEM((steps_a, rows, ds_width), BF16),
            pltpu.VMEM((max(steps_b, 1), rows, ds_width), BF16),
            pltpu.VMEM((n, 8, 128), F32),
            pltpu.VMEM((n, 8, width), F32),
            pltpu.VMEM((n, 8, 128), F32),
            dma,
            dma((teacher.shape[0],)),
            dma,
            dma((3, n, CHUNKS)),
            dma((n, CHUNKS)),
            dma((n, n)),
            dma((n,)),
            dma((2, steps_a, CHUNKS)),
            dma((2, steps_a, CHUNKS)),
            dma((n,)),
            dma((n,)),
            dma((n,)),
            dma((n,)),
            pltpu.VMEM((n // 2, rows, width), BF16),
            dma((n // 2,)),
            dma((n // 2,)),
        ],
        compiler_params=pltpu.CompilerParams(
            collective_id=0, has_side_effects=True, vmem_limit_bytes=56 * 1024 * 1024
        ),
    )(layer_map, boundaries, valid_counts, student_states[0], teacher, projector[0])
    return student_grad[None], projector_grad[None], loss[0, 0:1]


def solution(mesh):
    in_specs = (
        P("section", "dp", None),
        P("section", "dp", None),
        P("section", None, "dp"),
        P(),
        P(),
        P("dp"),
    )
    out_specs = (P("section", "dp", None), P("section", None, "dp"), P("section"))
    return jax.shard_map(
        per_device, mesh=mesh, in_specs=in_specs, out_specs=out_specs, check_vma=False
    )
```

```python
import functools

import jax
import jax.numpy as jnp
from jax import lax
from jax.experimental import pallas as pl
from jax.experimental.pallas import tpu as pltpu
from jax.sharding import PartitionSpec as P

loss_scale = 128.0
norm_eps = 1e-06
MESH = pl.DeviceIdType.MESH
F32, BF16 = jnp.float32, jnp.bfloat16
CHUNKS = 2
GRAD_TILES = 8


def from_behind(block, axis, distance):
    devices = range(lax.axis_size(axis))
    route = [(i - distance, i) for i in devices if i - distance in devices]
    return lax.ppermute(block, axis, route)


def lookup(table, index):
    places = jnp.arange(table.shape[0], dtype=jnp.int32)
    return jnp.sum(jnp.where(places == index, table, 0))


def relayed(teacher_states, layer_map, boundaries):
    sections = lax.axis_size("section")
    here = lax.axis_index("section")
    held_slots = teacher_states.shape[0]
    inner = boundaries[1:sections]
    owners = jnp.sum((inner[None, :] <= layer_map[:, None]).astype(jnp.int32), axis=1)
    first_layer = lookup(boundaries, here)

    def outgoing(offset):
        destination = here + offset
        inside = (destination >= 0) & (destination < sections)
        wanted = lookup(layer_map, destination)
        owner = lookup(owners, destination)
        place = jnp.clip(wanted - first_layer, 0, held_slots - 1)
        piece = lax.dynamic_index_in_dim(teacher_states, place, 0, keepdims=False)
        return jnp.where(inside & (owner == here), piece, jnp.zeros_like(piece))

    needed = here - lookup(owners, here)
    arrivals = []
    for offset in (-1, 1):
        stacked = jnp.stack([outgoing(offset), outgoing(2 * offset)])
        first_arrived = from_behind(stacked, "section", offset)
        second_arrived = from_behind(first_arrived[1:2], "section", offset)
        arrivals.append((offset, first_arrived[0]))
        arrivals.append((2 * offset, second_arrived[0]))
    hidden = outgoing(0)
    for offset, arrived in arrivals:
        hidden = jnp.where(needed == offset, arrived, hidden)
    return hidden


def send_to(here):
    return 2 - 2 * here + 5 * (here // 2)


def taken_from(here):
    return 1 + 2 * here - 5 * (here // 2)


def arrival_order(place, lines):
    order = []
    for step in range(lines - 1):
        sides = (place - 1 - step, place + 1 + step)
        order += [b for b in (sides if 2 * place < lines else sides[::-1]) if 0 <= b < lines]
    return order


def ring_start(n, steps_a, steps_b):
    lines = n // 2
    ring = [2 * p for p in range(lines)] + [2 * (n - 1 - p) + 1 for p in range(lines, n)]
    for step in range(1, lines - 1):
        ready = True
        for place in range(n):
            line, pair = ring[place] // 2, ring[place] % 2
            late = [b for k, b in enumerate(arrival_order(line, lines)) if k == 0 or k > step]
            late = [2 * b + 1 - pair for b in late]
            needed = [ring[(place + sign * offset) % n] for sign in (1, -1) for offset in (steps_a, -steps_b)]
            ready = ready and not set(late) & set(needed)
        if ready:
            return step
    return lines - 1


def main_kernel(n, direct, map_ref, bounds_ref, counts_ref, s_hbm, t_hbm, w_hbm, sg_ref, pg, loss_ref,
                teacher, count_ref, weights, stud, normed, tgt, proj, scaled, own, part_a, part_b, got_a, got_b,
                counts, losses, loss_out,
                in_sem, slab_sem, w_sem, ag_send, ag_recv, t_send, t_recv, rs_send, rs_recv,
                c_send, c_recv, l_send, l_recv, passing, p_send, p_recv):
    here = lax.axis_index("section")
    me = lax.axis_index("dp")
    rows, ds_width = s_hbm.shape
    width = weights.shape[1]
    half = rows // CHUNKS
    steps_a, steps_b = n // 2, n - 1 - n // 2
    teacher_width = width * n

    x, z = me % 2, me // 2
    position = z * (1 - x) + (n - 1 - z) * x
    sign = 1 - 2 * (here % 2)

    def at(offset):
        p = (position + sign * offset + 2 * n) % n
        low = 1 - p // (n // 2)
        return low * (2 * p) + (1 - low) * (2 * (n - 1 - p) + 1)

    after, before = at(1), at(-1)

    def block(index):
        return pl.ds(pl.multiple_of(index * rows, rows), rows)

    load_students = pltpu.make_async_copy(s_hbm, stud.at[block(me)], in_sem)
    load_students.start()
    held = teacher.shape[0]
    load_teacher = [
        pltpu.make_async_copy(t_hbm.at[slot], teacher.at[slot], slab_sem.at[slot]) for slot in range(held)
    ]
    barrier = pltpu.get_barrier_semaphore()
    for k in range(1, n):
        pl.semaphore_signal(barrier, inc=1, device_id=(here, (me + k) % n), device_id_type=MESH)
    expected = n - 1
    if direct:
        for k in range(n):
            pl.semaphore_signal(barrier, inc=1, device_id=(send_to(here), (me + k) % n), device_id_type=MESH)
            pl.semaphore_signal(barrier, inc=1, device_id=(taken_from(here), (me + k) % n), device_id_type=MESH)
        expected += 2 * n
    load_weights = pltpu.make_async_copy(w_hbm, weights, w_sem)
    for copy in load_teacher:
        copy.start()
    load_weights.start()
    count_ref[...] = jnp.full(count_ref.shape, counts_ref[0].astype(F32), F32)
    pl.semaphore_wait(barrier, expected)
    load_students.wait()

    pair, line = me % 2, me // 2
    partner = me + 1 - 2 * pair
    lines = n // 2

    def reached(place):
        return (line + lines - place) // lines

    def arrival_of(k):
        value = 0
        for place in range(lines):
            value = value + arrival_order(place, lines)[k] * (reached(place) - reached(place + 1))
        return value

    def piece_of(index, chunk):
        return stud.at[pl.ds(pl.multiple_of(index * rows + chunk * half, half), half)]

    UP, DOWN, ACROSS = 0, 1, 2
    targets_of = (me + 2, me - 2, me + 1 - 2 * pair)

    def ag_copy(way, index, step, chunk):
        return pltpu.make_async_remote_copy(
            src_ref=piece_of(index, chunk), dst_ref=piece_of(index, chunk),
            send_sem=ag_send.at[way, step, chunk], recv_sem=ag_recv.at[index, chunk],
            device_id=(here, targets_of[way]), device_id_type=MESH)

    def ag_arrival(index, chunk):
        return pltpu.make_async_remote_copy(
            src_ref=piece_of(index, chunk), dst_ref=piece_of(index, chunk),
            send_sem=ag_send.at[0, 0, chunk], recv_sem=ag_recv.at[index, chunk],
            device_id=(here, targets_of[2]), device_id_type=MESH)

    ag_steps = (steps_a, steps_b)
    sent = []
    sent_if = []

    def go(copy):
        copy.start()
        sent.append(copy)

    def go_if(condition, copy):
        pl.when(condition)(copy.start)
        sent_if.append((condition, copy))

    can_up, can_down = line < lines - 1, line > 0
    for chunk in range(CHUNKS):
        go_if(can_up, ag_copy(UP, me, 0, chunk))
        go_if(can_down, ag_copy(DOWN, me, 0, chunk))
        go(ag_copy(ACROSS, me, 0, chunk))

    def relay(step):
        below, above = me - 2 - 2 * step, me + 2 + 2 * step
        from_below, from_above = line - 1 - step >= 0, line + 1 + step < lines
        for chunk in range(CHUNKS):
            pl.when(from_below)(ag_arrival(below, chunk).wait_recv)
            go_if(from_below & can_up, ag_copy(UP, below, step + 1, chunk))
            pl.when(from_above)(ag_arrival(above, chunk).wait_recv)
            go_if(from_above & can_down, ag_copy(DOWN, above, step + 1, chunk))

    def relay_across(k):
        for chunk in range(CHUNKS):
            go(ag_copy(ACROSS, 2 * arrival_of(k) + pair, k + 1, chunk))

    def other_line(m):
        value, bit = 0, 1
        while bit < lines:
            mine = (line // bit) % 2
            flip = (m // bit) % 2
            value = value + bit * (mine + flip - 2 * mine * flip)
            bit *= 2
        return value

    def small(source, slots, send_sems, recv_sems, k):
        peer = (me + k) % n
        return pltpu.make_async_remote_copy(
            src_ref=source, dst_ref=slots.at[me], send_sem=send_sems.at[k], recv_sem=recv_sems.at[me],
            device_id=(here, peer), device_id_type=MESH)

    def small_arrival(slots, send_sems, recv_sems, k):
        peer = (me + k) % n
        return pltpu.make_async_remote_copy(
            src_ref=slots.at[peer], dst_ref=slots.at[peer], send_sem=send_sems.at[k],
            recv_sem=recv_sems.at[peer], device_id=(here, peer), device_id_type=MESH)

    for k in range(1, n):
        go(small(count_ref, counts, c_send, c_recv, k))
    counts[me] = count_ref[...]

    for copy in load_teacher:
        copy.wait()
    place = 0
    if direct:
        place = jnp.clip(map_ref[send_to(here)] - bounds_ref[here], 0, held - 1)
    squares = jnp.zeros((rows, 1), F32)
    for g in range(n):
        h = teacher[place, :, g * width:(g + 1) * width].astype(F32)
        squares += jnp.sum(h * h, axis=1, keepdims=True)
    inverse = lax.rsqrt(squares / teacher_width + norm_eps)
    for g in range(n):
        h = teacher[place, :, g * width:(g + 1) * width].astype(F32)
        normed[g] = (h * inverse).astype(BF16)
    taker = send_to(here) if direct else here

    def target_copy(source, owner, g):
        return pltpu.make_async_remote_copy(
            src_ref=source, dst_ref=tgt.at[block(owner)], send_sem=t_send.at[owner, g], recv_sem=t_recv.at[owner],
            device_id=(taker, g), device_id_type=MESH)

    def crossing(k):
        g = 2 * other_line(k) + 1 - pair
        return pltpu.make_async_remote_copy(
            src_ref=normed.at[g], dst_ref=passing.at[k], send_sem=p_send.at[k], recv_sem=p_recv.at[k],
            device_id=(here, partner), device_id_type=MESH)

    def own_target(k):
        g = 2 * other_line(k) + pair
        return target_copy(normed.at[g], me, g)

    def passed_target(k):
        g = 2 * other_line(k) + pair
        return target_copy(passing.at[k], partner, g)

    def target_arrival(index):
        return pltpu.make_async_remote_copy(
            src_ref=tgt.at[block(index)], dst_ref=tgt.at[block(index)], send_sem=t_send.at[0, index],
            recv_sem=t_recv.at[index], device_id=(taker, index), device_id_type=MESH)

    if not direct:
        tgt[block(me), :] = normed[me]
    far_first = range(lines - 1, 0, -1)
    for k in far_first:
        go(crossing(k))
    go(target_copy(normed.at[partner], me, partner))
    if direct:
        go(own_target(0))

    def project(index):
        proj[block(index), :] = jnp.dot(stud[block(index), :], weights[...], preferred_element_type=F32)

    row = lax.broadcasted_iota(jnp.int32, (rows, 1), 0).astype(F32)
    losses[me] = jnp.zeros(losses.shape[1:], F32)

    def total():
        value = counts[0][0:1, :]
        for b in range(1, n):
            value = value + counts[b][0:1, :]
        return value

    def residual(offset):
        index = at(offset)
        if direct or offset != 0:
            target_arrival(index).wait_recv()
        left = proj[block(index), :] - tgt[block(index), :].astype(F32)
        valid = jnp.where(row < counts[index][0:1, 0:1], 1.0, 0.0)
        kept = valid * left
        line = jnp.sum(kept * left, axis=0, keepdims=True)
        losses[me] += jnp.broadcast_to(line, losses.shape[1:])
        scaled[block(index), :] = (loss_scale / total()[:, 0:1] * kept).astype(BF16)

    def share(offset, into):
        own[into] = lax.dot_general(
            scaled[block(at(offset)), :], weights[...], (((1,), (1,)), ((), ())), preferred_element_type=F32)

    def rs_copy(direction, step, chunk):
        parts, gots = (part_a, got_a) if direction == 0 else (part_b, got_b)
        piece = pl.ds(chunk * half, half)
        return pltpu.make_async_remote_copy(
            src_ref=parts.at[step, piece], dst_ref=gots.at[step, piece],
            send_sem=rs_send.at[direction, step, chunk], recv_sem=rs_recv.at[direction, step, chunk],
            device_id=(here, after if direction == 0 else before), device_id_type=MESH)

    def grad_tile(tile):
        size = ds_width // GRAD_TILES
        left = stud[:, tile * size:(tile + 1) * size]
        pg[tile * size:(tile + 1) * size, :] = lax.dot_general(
            left, scaled[...], (((0,), (0,)), ((), ())), preferred_element_type=F32).astype(BF16)

    def advance(step, directions):
        for chunk in range(CHUNKS):
            piece = slice(chunk * half, (chunk + 1) * half)
            for direction in directions:
                if step >= ag_steps[direction]:
                    continue
                parts, gots = (part_a, got_a) if direction == 0 else (part_b, got_b)
                value = own[direction, piece, :]
                if step > 0:
                    rs_copy(direction, step - 1, chunk).wait_recv()
                    value = value + gots[step - 1, piece, :].astype(F32)
                parts[step, piece, :] = value.astype(BF16)
                go(rs_copy(direction, step, chunk))

    def prepare(step, direction):
        if step < ag_steps[direction]:
            offset = steps_a - step if direction == 0 else step - steps_b
            residual(offset)
            share(offset, direction)

    def project_across(source):
        index = 2 * source + 1 - pair
        for chunk in range(CHUNKS):
            ag_arrival(index, chunk).wait_recv()
        project(index)

    load_weights.wait()
    project(me)
    middle = min(1, lines - 2)
    for step in range(lines - 1):
        relay(step)
        if step == middle:
            for k in far_first:
                go(own_target(k))
        if step > 0:
            relay_across(step)
        if step == lines - 2:
            relay_across(0)
        project(2 * arrival_of(step) + pair)
        if step == 0:
            for k in range(1, n):
                small_arrival(counts, c_send, c_recv, k).wait_recv()
            project_across(line)
        if step == middle:
            for k in far_first:
                crossing(k).wait_recv()
                go(passed_target(k))
    start = ring_start(n, steps_a, steps_b)
    for step in range(1, lines):
        project_across(arrival_of(step % (lines - 1)))
        if step == start:
            prepare(0, 0)
            advance(0, (0,))
            prepare(0, 1)
            advance(0, (1,))

    for step in range(1, steps_a):
        prepare(step, 1)
        prepare(step, 0)
        if step == steps_a - 1:
            residual(0)
            share(0, 1)
        advance(step, (1, 0))

    line = losses[me][0:1, :]
    folded = jnp.sum(line, axis=1, keepdims=True)
    loss_out[me] = jnp.broadcast_to(folded, loss_out.shape[1:])
    grad_tile(0)
    for k in range(1, n):
        go(small(loss_out.at[me], loss_out, l_send, l_recv, k))
    for tile in range(1, GRAD_TILES):
        grad_tile(tile)

    for k in range(1, n):
        small_arrival(loss_out, l_send, l_recv, k).wait_recv()
    whole = loss_out[0][0:1, :]
    count = total()
    for b in range(1, n):
        whole = whole + loss_out[b][0:1, :]
    loss_ref[...] = jnp.broadcast_to(whole / (count * teacher_width), loss_ref.shape)

    for chunk in range(CHUNKS):
        piece = slice(chunk * half, (chunk + 1) * half)
        value = own[1, piece, :]
        rs_copy(0, steps_a - 1, chunk).wait_recv()
        value = value + got_a[steps_a - 1, piece, :].astype(F32)
        if steps_b > 0:
            rs_copy(1, steps_b - 1, chunk).wait_recv()
            value = value + got_b[steps_b - 1, piece, :].astype(F32)
        sg_ref[piece, :] = value.astype(BF16)
    for copy in sent:
        copy.wait_send()
    for condition, copy in sent_if:
        pl.when(condition)(copy.wait_send)


def per_device(student_states, teacher_states, projector, layer_map, boundaries, valid_counts):
    n = lax.axis_size("dp")
    rows, ds_width = student_states.shape[1:]
    width = projector.shape[2]
    direct = lax.axis_size("section") == 4
    teacher = teacher_states if direct else relayed(teacher_states, layer_map, boundaries)[None]
    steps_a, steps_b = n // 2, n - 1 - n // 2
    smem = pl.BlockSpec(memory_space=pltpu.SMEM)
    vmem = pl.BlockSpec(memory_space=pltpu.VMEM)
    anywhere = pl.BlockSpec(memory_space=pl.ANY)
    dma = pltpu.SemaphoreType.DMA
    student_grad, projector_grad, loss = pl.pallas_call(
        functools.partial(main_kernel, n, direct),
        out_shape=(
            pltpu.VMEM((rows, ds_width), BF16),
            pltpu.VMEM((ds_width, width), BF16),
            pltpu.VMEM((8, 128), F32),
        ),
        in_specs=[smem, smem, smem, anywhere, anywhere, anywhere],
        out_specs=(vmem, vmem, vmem),
        scratch_shapes=[
            pltpu.VMEM(teacher.shape, BF16),
            pltpu.VMEM((8, 128), F32),
            pltpu.VMEM((ds_width, width), BF16),
            pltpu.VMEM((n * rows, ds_width), BF16),
            pltpu.VMEM((n, rows, width), BF16),
            pltpu.VMEM((n * rows, width), BF16),
            pltpu.VMEM((n * rows, width), F32),
            pltpu.VMEM((n * rows, width), BF16),
            pltpu.VMEM((2, rows, ds_width), F32),
            pltpu.VMEM((steps_a, rows, ds_width), BF16),
            pltpu.VMEM((max(steps_b, 1), rows, ds_width), BF16),
            pltpu.VMEM((steps_a, rows, ds_width), BF16),
            pltpu.VMEM((max(steps_b, 1), rows, ds_width), BF16),
            pltpu.VMEM((n, 8, 128), F32),
            pltpu.VMEM((n, 8, width), F32),
            pltpu.VMEM((n, 8, 128), F32),
            dma,
            dma((teacher.shape[0],)),
            dma,
            dma((3, n, CHUNKS)),
            dma((n, CHUNKS)),
            dma((n, n)),
            dma((n,)),
            dma((2, steps_a, CHUNKS)),
            dma((2, steps_a, CHUNKS)),
            dma((n,)),
            dma((n,)),
            dma((n,)),
            dma((n,)),
            pltpu.VMEM((n // 2, rows, width), BF16),
            dma((n // 2,)),
            dma((n // 2,)),
        ],
        compiler_params=pltpu.CompilerParams(
            collective_id=0, has_side_effects=True, vmem_limit_bytes=56 * 1024 * 1024
        ),
    )(layer_map, boundaries, valid_counts, student_states[0], teacher, projector[0])
    return student_grad[None], projector_grad[None], loss[0, 0:1]


def solution(mesh):
    in_specs = (
        P("section", "dp", None),
        P("section", "dp", None),
        P("section", None, "dp"),
        P(),
        P(),
        P("dp"),
    )
    out_specs = (P("section", "dp", None), P("section", None, "dp"), P("section"))
    return jax.shard_map(
        per_device, mesh=mesh, in_specs=in_specs, out_specs=out_specs, check_vma=False
    )
```

```python
import functools

import jax
import jax.numpy as jnp
from jax import lax
from jax.experimental import pallas as pl
from jax.experimental.pallas import tpu as pltpu
from jax.sharding import PartitionSpec as P

loss_scale = 128.0
norm_eps = 1e-06
MESH = pl.DeviceIdType.MESH
F32, BF16 = jnp.float32, jnp.bfloat16
CHUNKS = 2
GRAD_TILES = 8


def from_behind(block, axis, distance):
    devices = range(lax.axis_size(axis))
    route = [(i - distance, i) for i in devices if i - distance in devices]
    return lax.ppermute(block, axis, route)


def lookup(table, index):
    places = jnp.arange(table.shape[0], dtype=jnp.int32)
    return jnp.sum(jnp.where(places == index, table, 0))


def relayed(teacher_states, layer_map, boundaries):
    sections = lax.axis_size("section")
    here = lax.axis_index("section")
    held_slots = teacher_states.shape[0]
    inner = boundaries[1:sections]
    owners = jnp.sum((inner[None, :] <= layer_map[:, None]).astype(jnp.int32), axis=1)
    first_layer = lookup(boundaries, here)

    def outgoing(offset):
        destination = here + offset
        inside = (destination >= 0) & (destination < sections)
        wanted = lookup(layer_map, destination)
        owner = lookup(owners, destination)
        place = jnp.clip(wanted - first_layer, 0, held_slots - 1)
        piece = lax.dynamic_index_in_dim(teacher_states, place, 0, keepdims=False)
        return jnp.where(inside & (owner == here), piece, jnp.zeros_like(piece))

    needed = here - lookup(owners, here)
    arrivals = []
    for offset in (-1, 1):
        stacked = jnp.stack([outgoing(offset), outgoing(2 * offset)])
        first_arrived = from_behind(stacked, "section", offset)
        second_arrived = from_behind(first_arrived[1:2], "section", offset)
        arrivals.append((offset, first_arrived[0]))
        arrivals.append((2 * offset, second_arrived[0]))
    hidden = outgoing(0)
    for offset, arrived in arrivals:
        hidden = jnp.where(needed == offset, arrived, hidden)
    return hidden


def send_to(here):
    return 2 - 2 * here + 5 * (here // 2)


def taken_from(here):
    return 1 + 2 * here - 5 * (here // 2)


def arrival_order(place, lines):
    order = []
    for step in range(lines - 1):
        sides = (place - 1 - step, place + 1 + step)
        order += [b for b in (sides if 2 * place < lines else sides[::-1]) if 0 <= b < lines]
    return order


def ring_start(n, steps_a, steps_b):
    lines = n // 2
    ring = [2 * p for p in range(lines)] + [2 * (n - 1 - p) + 1 for p in range(lines, n)]
    for step in range(1, lines - 1):
        ready = True
        for place in range(n):
            line, pair = ring[place] // 2, ring[place] % 2
            late = [b for k, b in enumerate(arrival_order(line, lines)) if k == 0 or k > step]
            late = [2 * b + 1 - pair for b in late]
            needed = [ring[(place + sign * offset) % n] for sign in (1, -1) for offset in (steps_a, -steps_b)]
            ready = ready and not set(late) & set(needed)
        if ready:
            return step
    return lines - 1


def main_kernel(n, direct, map_ref, bounds_ref, counts_ref, s_hbm, t_hbm, w_hbm, sg_ref, pg, loss_ref,
                teacher, count_ref, weights, stud, normed, tgt, proj, scaled, own, part_a, part_b, got_a, got_b,
                counts, losses, loss_out,
                in_sem, slab_sem, w_sem, ag_send, ag_recv, t_send, t_recv, rs_send, rs_recv,
                c_send, c_recv, l_send, l_recv, passing, p_send, p_recv, rounds):
    here = lax.axis_index("section")
    me = lax.axis_index("dp")
    rows, ds_width = s_hbm.shape
    width = weights.shape[1]
    half = rows // CHUNKS
    steps_a, steps_b = n // 2, n - 1 - n // 2
    teacher_width = width * n

    pair, line = me % 2, me // 2
    partner = me + 1 - 2 * pair
    lines = n // 2
    can_up, can_down = line < lines - 1, line > 0
    x, z = me % 2, me // 2
    position = z * (1 - x) + (n - 1 - z) * x
    sign = 1 - 2 * (here % 2)

    def at(offset):
        p = (position + sign * offset + 2 * n) % n
        low = 1 - p // (n // 2)
        return low * (2 * p) + (1 - low) * (2 * (n - 1 - p) + 1)

    after, before = at(1), at(-1)

    def block(index):
        return pl.ds(pl.multiple_of(index * rows, rows), rows)

    load_students = pltpu.make_async_copy(s_hbm, stud.at[block(me)], in_sem)
    load_students.start()
    held = teacher.shape[0]
    load_teacher = [
        pltpu.make_async_copy(t_hbm.at[slot], teacher.at[slot], slab_sem.at[slot]) for slot in range(held)
    ]
    barrier = pltpu.get_barrier_semaphore()
    near = 2 - line // (lines - 1) + (line + lines - 1) // lines + 2 * direct

    def greet(semaphore):
        def signal(section, device):
            pl.semaphore_signal(semaphore, inc=1, device_id=(section, device), device_id_type=MESH)

        signal(here, partner)
        pl.when(can_up)(lambda: signal(here, me + 2))
        pl.when(can_down)(lambda: signal(here, me - 2))
        if direct:
            signal(send_to(here), me)
            signal(taken_from(here), me)

    def next_round(k):
        if k > 0:
            pl.semaphore_wait(rounds.at[k - 1], near)
        if k < lines - 1:
            greet(rounds.at[k])

    load_weights = pltpu.make_async_copy(w_hbm, weights, w_sem)
    greet(barrier)
    for copy in load_teacher:
        copy.start()
    load_weights.start()
    count_ref[...] = jnp.full(count_ref.shape, counts_ref[0].astype(F32), F32)
    pl.semaphore_wait(barrier, near)
    load_students.wait()


    def reached(place):
        return (line + lines - place) // lines

    def arrival_of(k):
        value = 0
        for place in range(lines):
            value = value + arrival_order(place, lines)[k] * (reached(place) - reached(place + 1))
        return value

    def piece_of(index, chunk):
        return stud.at[pl.ds(pl.multiple_of(index * rows + chunk * half, half), half)]

    UP, DOWN, ACROSS = 0, 1, 2
    targets_of = (me + 2, me - 2, me + 1 - 2 * pair)

    def ag_copy(way, index, step, chunk):
        return pltpu.make_async_remote_copy(
            src_ref=piece_of(index, chunk), dst_ref=piece_of(index, chunk),
            send_sem=ag_send.at[way, step, chunk], recv_sem=ag_recv.at[index, chunk],
            device_id=(here, targets_of[way]), device_id_type=MESH)

    def ag_arrival(index, chunk):
        return pltpu.make_async_remote_copy(
            src_ref=piece_of(index, chunk), dst_ref=piece_of(index, chunk),
            send_sem=ag_send.at[0, 0, chunk], recv_sem=ag_recv.at[index, chunk],
            device_id=(here, targets_of[2]), device_id_type=MESH)

    ag_steps = (steps_a, steps_b)
    sent = []
    sent_if = []

    def go(copy):
        copy.start()
        sent.append(copy)

    def go_if(condition, copy):
        pl.when(condition)(copy.start)
        sent_if.append((condition, copy))

    for chunk in range(CHUNKS):
        go_if(can_up, ag_copy(UP, me, 0, chunk))
        go_if(can_down, ag_copy(DOWN, me, 0, chunk))
        go(ag_copy(ACROSS, me, 0, chunk))

    def relay(step):
        below, above = me - 2 - 2 * step, me + 2 + 2 * step
        from_below, from_above = line - 1 - step >= 0, line + 1 + step < lines
        for chunk in range(CHUNKS):
            pl.when(from_below)(ag_arrival(below, chunk).wait_recv)
            go_if(from_below & can_up, ag_copy(UP, below, step + 1, chunk))
            pl.when(from_above)(ag_arrival(above, chunk).wait_recv)
            go_if(from_above & can_down, ag_copy(DOWN, above, step + 1, chunk))

    def relay_across(k):
        for chunk in range(CHUNKS):
            go(ag_copy(ACROSS, 2 * arrival_of(k) + pair, k + 1, chunk))

    def other_line(m):
        value, bit = 0, 1
        while bit < lines:
            mine = (line // bit) % 2
            flip = (m // bit) % 2
            value = value + bit * (mine + flip - 2 * mine * flip)
            bit *= 2
        return value

    def small(source, slots, send_sems, recv_sems, k):
        peer = (me + k) % n
        return pltpu.make_async_remote_copy(
            src_ref=source, dst_ref=slots.at[me], send_sem=send_sems.at[k], recv_sem=recv_sems.at[me],
            device_id=(here, peer), device_id_type=MESH)

    def small_arrival(slots, send_sems, recv_sems, k):
        peer = (me + k) % n
        return pltpu.make_async_remote_copy(
            src_ref=slots.at[peer], dst_ref=slots.at[peer], send_sem=send_sems.at[k],
            recv_sem=recv_sems.at[peer], device_id=(here, peer), device_id_type=MESH)

    counts[me] = count_ref[...]
    next_round(0)

    for copy in load_teacher:
        copy.wait()
    place = 0
    if direct:
        place = jnp.clip(map_ref[send_to(here)] - bounds_ref[here], 0, held - 1)
    squares = jnp.zeros((rows, 1), F32)
    for g in range(n):
        h = teacher[place, :, g * width:(g + 1) * width].astype(F32)
        squares += jnp.sum(h * h, axis=1, keepdims=True)
    next_round(1)
    inverse = lax.rsqrt(squares / teacher_width + norm_eps)
    for g in range(n):
        h = teacher[place, :, g * width:(g + 1) * width].astype(F32)
        normed[g] = (h * inverse).astype(BF16)
    taker = send_to(here) if direct else here

    def target_copy(source, owner, g):
        return pltpu.make_async_remote_copy(
            src_ref=source, dst_ref=tgt.at[block(owner)], send_sem=t_send.at[owner, g], recv_sem=t_recv.at[owner],
            device_id=(taker, g), device_id_type=MESH)

    def crossing(k):
        g = 2 * other_line(k) + 1 - pair
        return pltpu.make_async_remote_copy(
            src_ref=normed.at[g], dst_ref=passing.at[k], send_sem=p_send.at[k], recv_sem=p_recv.at[k],
            device_id=(here, partner), device_id_type=MESH)

    def own_target(k):
        g = 2 * other_line(k) + pair
        return target_copy(normed.at[g], me, g)

    def passed_target(k):
        g = 2 * other_line(k) + pair
        return target_copy(passing.at[k], partner, g)

    def target_arrival(index):
        return pltpu.make_async_remote_copy(
            src_ref=tgt.at[block(index)], dst_ref=tgt.at[block(index)], send_sem=t_send.at[0, index],
            recv_sem=t_recv.at[index], device_id=(taker, index), device_id_type=MESH)

    if not direct:
        tgt[block(me), :] = normed[me]
    far_first = range(lines - 1, 0, -1)
    for k in far_first:
        go(crossing(k))
    for k in range(2, lines):
        next_round(k)
    go(target_copy(normed.at[partner], me, partner))
    if direct:
        go(own_target(0))

    def project(index):
        proj[block(index), :] = jnp.dot(stud[block(index), :], weights[...], preferred_element_type=F32)

    row = lax.broadcasted_iota(jnp.int32, (rows, 1), 0).astype(F32)
    losses[me] = jnp.zeros(losses.shape[1:], F32)

    def total():
        value = counts[0][0:1, :]
        for b in range(1, n):
            value = value + counts[b][0:1, :]
        return value

    def residual(offset):
        index = at(offset)
        if direct or offset != 0:
            target_arrival(index).wait_recv()
        left = proj[block(index), :] - tgt[block(index), :].astype(F32)
        valid = jnp.where(row < counts[index][0:1, 0:1], 1.0, 0.0)
        kept = valid * left
        line = jnp.sum(kept * left, axis=0, keepdims=True)
        losses[me] += jnp.broadcast_to(line, losses.shape[1:])
        scaled[block(index), :] = (loss_scale / total()[:, 0:1] * kept).astype(BF16)

    def share(offset, into):
        own[into] = lax.dot_general(
            scaled[block(at(offset)), :], weights[...], (((1,), (1,)), ((), ())), preferred_element_type=F32)

    def rs_copy(direction, step, chunk):
        parts, gots = (part_a, got_a) if direction == 0 else (part_b, got_b)
        piece = pl.ds(chunk * half, half)
        return pltpu.make_async_remote_copy(
            src_ref=parts.at[step, piece], dst_ref=gots.at[step, piece],
            send_sem=rs_send.at[direction, step, chunk], recv_sem=rs_recv.at[direction, step, chunk],
            device_id=(here, after if direction == 0 else before), device_id_type=MESH)

    def grad_tile(tile):
        size = ds_width // GRAD_TILES
        left = stud[:, tile * size:(tile + 1) * size]
        pg[tile * size:(tile + 1) * size, :] = lax.dot_general(
            left, scaled[...], (((0,), (0,)), ((), ())), preferred_element_type=F32).astype(BF16)

    def advance(step, directions):
        for chunk in range(CHUNKS):
            piece = slice(chunk * half, (chunk + 1) * half)
            for direction in directions:
                if step >= ag_steps[direction]:
                    continue
                parts, gots = (part_a, got_a) if direction == 0 else (part_b, got_b)
                value = own[direction, piece, :]
                if step > 0:
                    rs_copy(direction, step - 1, chunk).wait_recv()
                    value = value + gots[step - 1, piece, :].astype(F32)
                parts[step, piece, :] = value.astype(BF16)
                go(rs_copy(direction, step, chunk))

    def prepare(step, direction):
        if step < ag_steps[direction]:
            offset = steps_a - step if direction == 0 else step - steps_b
            residual(offset)
            share(offset, direction)

    def project_across(source):
        index = 2 * source + 1 - pair
        for chunk in range(CHUNKS):
            ag_arrival(index, chunk).wait_recv()
        project(index)

    load_weights.wait()
    project(me)
    middle = min(1, lines - 2)
    for step in range(lines - 1):
        relay(step)
        if step == 0:
            for k in range(1, n):
                go(small(count_ref, counts, c_send, c_recv, k))
        if step == middle:
            for k in far_first:
                go(own_target(k))
        if step > 0:
            relay_across(step)
        if step == lines - 2:
            relay_across(0)
        project(2 * arrival_of(step) + pair)
        if step == 0:
            project_across(line)
        if step == middle:
            for k in far_first:
                crossing(k).wait_recv()
                go(passed_target(k))
    start = ring_start(n, steps_a, steps_b)
    for k in range(1, n):
        small_arrival(counts, c_send, c_recv, k).wait_recv()
    for step in range(1, lines):
        project_across(arrival_of(step % (lines - 1)))
        if step == start:
            prepare(0, 0)
            advance(0, (0,))
            prepare(0, 1)
            advance(0, (1,))

    for step in range(1, steps_a):
        prepare(step, 1)
        prepare(step, 0)
        if step == steps_a - 1:
            residual(0)
            share(0, 1)
        advance(step, (1, 0))

    line = losses[me][0:1, :]
    folded = jnp.sum(line, axis=1, keepdims=True)
    loss_out[me] = jnp.broadcast_to(folded, loss_out.shape[1:])
    grad_tile(0)
    for k in range(1, n):
        go(small(loss_out.at[me], loss_out, l_send, l_recv, k))
    for tile in range(1, GRAD_TILES):
        grad_tile(tile)

    for k in range(1, n):
        small_arrival(loss_out, l_send, l_recv, k).wait_recv()
    whole = loss_out[0][0:1, :]
    count = total()
    for b in range(1, n):
        whole = whole + loss_out[b][0:1, :]
    loss_ref[...] = jnp.broadcast_to(whole / (count * teacher_width), loss_ref.shape)

    for chunk in range(CHUNKS):
        piece = slice(chunk * half, (chunk + 1) * half)
        value = own[1, piece, :]
        rs_copy(0, steps_a - 1, chunk).wait_recv()
        value = value + got_a[steps_a - 1, piece, :].astype(F32)
        if steps_b > 0:
            rs_copy(1, steps_b - 1, chunk).wait_recv()
            value = value + got_b[steps_b - 1, piece, :].astype(F32)
        sg_ref[piece, :] = value.astype(BF16)
    for copy in sent:
        copy.wait_send()
    for condition, copy in sent_if:
        pl.when(condition)(copy.wait_send)


def per_device(student_states, teacher_states, projector, layer_map, boundaries, valid_counts):
    n = lax.axis_size("dp")
    rows, ds_width = student_states.shape[1:]
    width = projector.shape[2]
    direct = lax.axis_size("section") == 4
    teacher = teacher_states if direct else relayed(teacher_states, layer_map, boundaries)[None]
    steps_a, steps_b = n // 2, n - 1 - n // 2
    smem = pl.BlockSpec(memory_space=pltpu.SMEM)
    vmem = pl.BlockSpec(memory_space=pltpu.VMEM)
    anywhere = pl.BlockSpec(memory_space=pl.ANY)
    dma = pltpu.SemaphoreType.DMA
    student_grad, projector_grad, loss = pl.pallas_call(
        functools.partial(main_kernel, n, direct),
        out_shape=(
            pltpu.VMEM((rows, ds_width), BF16),
            pltpu.VMEM((ds_width, width), BF16),
            pltpu.VMEM((8, 128), F32),
        ),
        in_specs=[smem, smem, smem, anywhere, anywhere, anywhere],
        out_specs=(vmem, vmem, vmem),
        scratch_shapes=[
            pltpu.VMEM(teacher.shape, BF16),
            pltpu.VMEM((8, 128), F32),
            pltpu.VMEM((ds_width, width), BF16),
            pltpu.VMEM((n * rows, ds_width), BF16),
            pltpu.VMEM((n, rows, width), BF16),
            pltpu.VMEM((n * rows, width), BF16),
            pltpu.VMEM((n * rows, width), F32),
            pltpu.VMEM((n * rows, width), BF16),
            pltpu.VMEM((2, rows, ds_width), F32),
            pltpu.VMEM((steps_a, rows, ds_width), BF16),
            pltpu.VMEM((max(steps_b, 1), rows, ds_width), BF16),
            pltpu.VMEM((steps_a, rows, ds_width), BF16),
            pltpu.VMEM((max(steps_b, 1), rows, ds_width), BF16),
            pltpu.VMEM((n, 8, 128), F32),
            pltpu.VMEM((n, 8, width), F32),
            pltpu.VMEM((n, 8, 128), F32),
            dma,
            dma((teacher.shape[0],)),
            dma,
            dma((3, n, CHUNKS)),
            dma((n, CHUNKS)),
            dma((n, n)),
            dma((n,)),
            dma((2, steps_a, CHUNKS)),
            dma((2, steps_a, CHUNKS)),
            dma((n,)),
            dma((n,)),
            dma((n,)),
            dma((n,)),
            pltpu.VMEM((n // 2, rows, width), BF16),
            dma((n // 2,)),
            dma((n // 2,)),
            pltpu.SemaphoreType.REGULAR((n // 2 - 1,)),
        ],
        compiler_params=pltpu.CompilerParams(
            collective_id=0, has_side_effects=True, vmem_limit_bytes=56 * 1024 * 1024
        ),
    )(layer_map, boundaries, valid_counts, student_states[0], teacher, projector[0])
    return student_grad[None], projector_grad[None], loss[0, 0:1]


def solution(mesh):
    in_specs = (
        P("section", "dp", None),
        P("section", "dp", None),
        P("section", None, "dp"),
        P(),
        P(),
        P("dp"),
    )
    out_specs = (P("section", "dp", None), P("section", None, "dp"), P("section"))
    return jax.shard_map(
        per_device, mesh=mesh, in_specs=in_specs, out_specs=out_specs, check_vma=False
    )
```

```python
import functools

import jax
import jax.numpy as jnp
from jax import lax
from jax.experimental import pallas as pl
from jax.experimental.pallas import tpu as pltpu
from jax.sharding import PartitionSpec as P

loss_scale = 128.0
norm_eps = 1e-06
MESH = pl.DeviceIdType.MESH
F32, BF16 = jnp.float32, jnp.bfloat16
CHUNKS = 2
GRAD_TILES = 8


def from_behind(block, axis, distance):
    devices = range(lax.axis_size(axis))
    route = [(i - distance, i) for i in devices if i - distance in devices]
    return lax.ppermute(block, axis, route)


def lookup(table, index):
    places = jnp.arange(table.shape[0], dtype=jnp.int32)
    return jnp.sum(jnp.where(places == index, table, 0))


def relayed(teacher_states, layer_map, boundaries):
    sections = lax.axis_size("section")
    here = lax.axis_index("section")
    held_slots = teacher_states.shape[0]
    inner = boundaries[1:sections]
    owners = jnp.sum((inner[None, :] <= layer_map[:, None]).astype(jnp.int32), axis=1)
    first_layer = lookup(boundaries, here)

    def outgoing(offset):
        destination = here + offset
        inside = (destination >= 0) & (destination < sections)
        wanted = lookup(layer_map, destination)
        owner = lookup(owners, destination)
        place = jnp.clip(wanted - first_layer, 0, held_slots - 1)
        piece = lax.dynamic_index_in_dim(teacher_states, place, 0, keepdims=False)
        return jnp.where(inside & (owner == here), piece, jnp.zeros_like(piece))

    needed = here - lookup(owners, here)
    arrivals = []
    for offset in (-1, 1):
        stacked = jnp.stack([outgoing(offset), outgoing(2 * offset)])
        first_arrived = from_behind(stacked, "section", offset)
        second_arrived = from_behind(first_arrived[1:2], "section", offset)
        arrivals.append((offset, first_arrived[0]))
        arrivals.append((2 * offset, second_arrived[0]))
    hidden = outgoing(0)
    for offset, arrived in arrivals:
        hidden = jnp.where(needed == offset, arrived, hidden)
    return hidden


def send_to(here):
    return 2 - 2 * here + 5 * (here // 2)


def taken_from(here):
    return 1 + 2 * here - 5 * (here // 2)


def arrival_order(place, lines):
    order = []
    for step in range(lines - 1):
        sides = (place - 1 - step, place + 1 + step)
        order += [b for b in (sides if 2 * place < lines else sides[::-1]) if 0 <= b < lines]
    return order


def ring_start(n, steps_a, steps_b):
    lines = n // 2
    ring = [2 * p for p in range(lines)] + [2 * (n - 1 - p) + 1 for p in range(lines, n)]
    for step in range(1, lines - 1):
        ready = True
        for place in range(n):
            line, pair = ring[place] // 2, ring[place] % 2
            late = [b for k, b in enumerate(arrival_order(line, lines)) if k == 0 or k > step]
            late = [2 * b + 1 - pair for b in late]
            needed = [ring[(place + sign * offset) % n] for sign in (1, -1) for offset in (steps_a, -steps_b)]
            ready = ready and not set(late) & set(needed)
        if ready:
            return step
    return lines - 1


def main_kernel(n, direct, map_ref, bounds_ref, counts_ref, s_hbm, t_hbm, w_hbm, sg_ref, pg, loss_ref,
                teacher, count_ref, weights, stud, normed, tgt, proj, scaled, own, part_a, part_b, got_a, got_b,
                counts, losses, loss_out,
                in_sem, slab_sem, w_sem, ag_send, ag_recv, t_send, t_recv, rs_send, rs_recv,
                c_send, c_recv, l_send, l_recv, passing, p_send, p_recv, rounds):
    here = lax.axis_index("section")
    me = lax.axis_index("dp")
    rows, ds_width = s_hbm.shape
    width = weights.shape[1]
    half = rows // CHUNKS
    steps_a, steps_b = n // 2, n - 1 - n // 2
    teacher_width = width * n

    pair, line = me % 2, me // 2
    partner = me + 1 - 2 * pair
    lines = n // 2
    can_up, can_down = line < lines - 1, line > 0
    x, z = me % 2, me // 2
    position = z * (1 - x) + (n - 1 - z) * x
    sign = 1 - 2 * (here % 2)

    def at(offset):
        p = (position + sign * offset + 2 * n) % n
        low = 1 - p // (n // 2)
        return low * (2 * p) + (1 - low) * (2 * (n - 1 - p) + 1)

    after, before = at(1), at(-1)

    def block(index):
        return pl.ds(pl.multiple_of(index * rows, rows), rows)

    load_students = pltpu.make_async_copy(s_hbm, stud.at[block(me)], in_sem)
    load_students.start()
    held = teacher.shape[0]
    load_teacher = [
        pltpu.make_async_copy(t_hbm.at[slot], teacher.at[slot], slab_sem.at[slot]) for slot in range(held)
    ]
    barrier = pltpu.get_barrier_semaphore()
    near = 2 - line // (lines - 1) + (line + lines - 1) // lines + 2 * direct

    def greet(semaphore):
        def signal(section, device):
            pl.semaphore_signal(semaphore, inc=1, device_id=(section, device), device_id_type=MESH)

        signal(here, partner)
        pl.when(can_up)(lambda: signal(here, me + 2))
        pl.when(can_down)(lambda: signal(here, me - 2))
        if direct:
            signal(send_to(here), me)
            signal(taken_from(here), me)

    def next_round(k):
        if k > 0:
            pl.semaphore_wait(rounds.at[k - 1], near)
        if k < lines - 1:
            greet(rounds.at[k])

    load_weights = pltpu.make_async_copy(w_hbm, weights, w_sem)
    greet(barrier)
    for copy in load_teacher:
        copy.start()
    load_weights.start()
    count_ref[...] = jnp.full(count_ref.shape, counts_ref[0].astype(F32), F32)
    pl.semaphore_wait(barrier, near)
    load_students.wait()


    def reached(place):
        return (line + lines - place) // lines

    def arrival_of(k):
        value = 0
        for place in range(lines):
            value = value + arrival_order(place, lines)[k] * (reached(place) - reached(place + 1))
        return value

    def piece_of(index, chunk):
        return stud.at[pl.ds(pl.multiple_of(index * rows + chunk * half, half), half)]

    UP, DOWN, ACROSS = 0, 1, 2
    targets_of = (me + 2, me - 2, me + 1 - 2 * pair)

    def ag_copy(way, index, step, chunk):
        return pltpu.make_async_remote_copy(
            src_ref=piece_of(index, chunk), dst_ref=piece_of(index, chunk),
            send_sem=ag_send.at[way, step, chunk], recv_sem=ag_recv.at[index, chunk],
            device_id=(here, targets_of[way]), device_id_type=MESH)

    def ag_arrival(index, chunk):
        return pltpu.make_async_remote_copy(
            src_ref=piece_of(index, chunk), dst_ref=piece_of(index, chunk),
            send_sem=ag_send.at[0, 0, chunk], recv_sem=ag_recv.at[index, chunk],
            device_id=(here, targets_of[2]), device_id_type=MESH)

    ag_steps = (steps_a, steps_b)
    sent = []
    sent_if = []

    def go(copy):
        copy.start()
        sent.append(copy)

    def go_if(condition, copy):
        pl.when(condition)(copy.start)
        sent_if.append((condition, copy))

    for chunk in range(CHUNKS):
        go_if(can_up, ag_copy(UP, me, 0, chunk))
        go_if(can_down, ag_copy(DOWN, me, 0, chunk))
        go(ag_copy(ACROSS, me, 0, chunk))

    def relay(step):
        below, above = me - 2 - 2 * step, me + 2 + 2 * step
        from_below, from_above = line - 1 - step >= 0, line + 1 + step < lines
        for chunk in range(CHUNKS):
            pl.when(from_below)(ag_arrival(below, chunk).wait_recv)
            go_if(from_below & can_up, ag_copy(UP, below, step + 1, chunk))
            pl.when(from_above)(ag_arrival(above, chunk).wait_recv)
            go_if(from_above & can_down, ag_copy(DOWN, above, step + 1, chunk))

    def relay_across(k):
        for chunk in range(CHUNKS):
            go(ag_copy(ACROSS, 2 * arrival_of(k) + pair, k + 1, chunk))

    def other_line(m):
        value, bit = 0, 1
        while bit < lines:
            mine = (line // bit) % 2
            flip = (m // bit) % 2
            value = value + bit * (mine + flip - 2 * mine * flip)
            bit *= 2
        return value

    def small(source, slots, send_sems, recv_sems, k):
        peer = (me + k) % n
        return pltpu.make_async_remote_copy(
            src_ref=source, dst_ref=slots.at[me], send_sem=send_sems.at[k], recv_sem=recv_sems.at[me],
            device_id=(here, peer), device_id_type=MESH)

    def small_arrival(slots, send_sems, recv_sems, k):
        peer = (me + k) % n
        return pltpu.make_async_remote_copy(
            src_ref=slots.at[peer], dst_ref=slots.at[peer], send_sem=send_sems.at[k],
            recv_sem=recv_sems.at[peer], device_id=(here, peer), device_id_type=MESH)

    counts[me] = count_ref[...]
    next_round(0)

    for copy in load_teacher:
        copy.wait()
    place = 0
    if direct:
        place = jnp.clip(map_ref[send_to(here)] - bounds_ref[here], 0, held - 1)
    squares = jnp.zeros((rows, 1), F32)
    for g in range(n):
        h = teacher[place, :, g * width:(g + 1) * width].astype(F32)
        squares += jnp.sum(h * h, axis=1, keepdims=True)
    next_round(1)
    inverse = lax.rsqrt(squares / teacher_width + norm_eps)
    for g in range(n):
        h = teacher[place, :, g * width:(g + 1) * width].astype(F32)
        normed[g] = (h * inverse).astype(BF16)
    taker = send_to(here) if direct else here

    def target_copy(source, owner, g):
        return pltpu.make_async_remote_copy(
            src_ref=source, dst_ref=tgt.at[block(owner)], send_sem=t_send.at[owner, g], recv_sem=t_recv.at[owner],
            device_id=(taker, g), device_id_type=MESH)

    def crossing(k):
        g = 2 * other_line(k) + 1 - pair
        return pltpu.make_async_remote_copy(
            src_ref=normed.at[g], dst_ref=passing.at[k], send_sem=p_send.at[k], recv_sem=p_recv.at[k],
            device_id=(here, partner), device_id_type=MESH)

    def own_target(k):
        g = 2 * other_line(k) + pair
        return target_copy(normed.at[g], me, g)

    def passed_target(k):
        g = 2 * other_line(k) + pair
        return target_copy(passing.at[k], partner, g)

    def target_arrival(index):
        return pltpu.make_async_remote_copy(
            src_ref=tgt.at[block(index)], dst_ref=tgt.at[block(index)], send_sem=t_send.at[0, index],
            recv_sem=t_recv.at[index], device_id=(taker, index), device_id_type=MESH)

    if not direct:
        tgt[block(me), :] = normed[me]
    far_first = range(lines - 1, 0, -1)
    for k in far_first:
        go(crossing(k))
    for k in range(2, lines):
        next_round(k)
    go(target_copy(normed.at[partner], me, partner))
    if direct:
        go(own_target(0))

    def project(index):
        proj[block(index), :] = jnp.dot(stud[block(index), :], weights[...], preferred_element_type=F32)

    row = lax.broadcasted_iota(jnp.int32, (rows, 1), 0).astype(F32)
    losses[me] = jnp.zeros(losses.shape[1:], F32)

    def total():
        value = counts[0][0:1, :]
        for b in range(1, n):
            value = value + counts[b][0:1, :]
        return value

    def residual(offset):
        index = at(offset)
        if direct or offset != 0:
            target_arrival(index).wait_recv()
        left = proj[block(index), :] - tgt[block(index), :].astype(F32)
        valid = jnp.where(row < counts[index][0:1, 0:1], 1.0, 0.0)
        kept = valid * left
        line = jnp.sum(kept * left, axis=0, keepdims=True)
        losses[me] += jnp.broadcast_to(line, losses.shape[1:])
        scaled[block(index), :] = (loss_scale / total()[:, 0:1] * kept).astype(BF16)

    def share(offset, into):
        own[into] = lax.dot_general(
            scaled[block(at(offset)), :], weights[...], (((1,), (1,)), ((), ())), preferred_element_type=F32)

    def rs_copy(direction, step, chunk):
        parts, gots = (part_a, got_a) if direction == 0 else (part_b, got_b)
        piece = pl.ds(chunk * half, half)
        return pltpu.make_async_remote_copy(
            src_ref=parts.at[step, piece], dst_ref=gots.at[step, piece],
            send_sem=rs_send.at[direction, step, chunk], recv_sem=rs_recv.at[direction, step, chunk],
            device_id=(here, after if direction == 0 else before), device_id_type=MESH)

    def grad_tile(tile):
        size = ds_width // GRAD_TILES
        left = stud[:, tile * size:(tile + 1) * size]
        pg[tile * size:(tile + 1) * size, :] = lax.dot_general(
            left, scaled[...], (((0,), (0,)), ((), ())), preferred_element_type=F32).astype(BF16)

    def advance(step, directions):
        for chunk in range(CHUNKS):
            piece = slice(chunk * half, (chunk + 1) * half)
            for direction in directions:
                if step >= ag_steps[direction]:
                    continue
                parts, gots = (part_a, got_a) if direction == 0 else (part_b, got_b)
                value = own[direction, piece, :]
                if step > 0:
                    rs_copy(direction, step - 1, chunk).wait_recv()
                    value = value + gots[step - 1, piece, :].astype(F32)
                parts[step, piece, :] = value.astype(BF16)
                go(rs_copy(direction, step, chunk))

    def prepare(step, direction):
        if step < ag_steps[direction]:
            offset = steps_a - step if direction == 0 else step - steps_b
            residual(offset)
            share(offset, direction)

    def project_across(source):
        index = 2 * source + 1 - pair
        for chunk in range(CHUNKS):
            ag_arrival(index, chunk).wait_recv()
        project(index)

    load_weights.wait()
    project(me)
    middle = min(1, lines - 2)
    for step in range(lines - 1):
        relay(step)
        if step == 0:
            for k in range(1, n):
                go(small(count_ref, counts, c_send, c_recv, k))
        if step == middle:
            for k in far_first:
                go(own_target(k))
        if step > 0:
            relay_across(step)
        if step == lines - 2:
            relay_across(0)
        project(2 * arrival_of(step) + pair)
        if step == 0:
            project_across(line)
        if step == middle:
            for k in far_first:
                crossing(k).wait_recv()
                go(passed_target(k))
    start = ring_start(n, steps_a, steps_b)
    for k in range(1, n):
        small_arrival(counts, c_send, c_recv, k).wait_recv()
    for step in range(1, lines):
        project_across(arrival_of(step % (lines - 1)))
        if step == start:
            prepare(0, 0)
            advance(0, (0,))
            prepare(0, 1)
            advance(0, (1,))

    for step in range(1, steps_a):
        prepare(step, 1)
        prepare(step, 0)
        if step == steps_a - 1:
            residual(0)
            share(0, 1)
        advance(step, (1, 0))

    line = losses[me][0:1, :]
    folded = jnp.sum(line, axis=1, keepdims=True)
    loss_out[me] = jnp.broadcast_to(folded, loss_out.shape[1:])
    grad_tile(0)
    for k in range(1, n):
        go(small(loss_out.at[me], loss_out, l_send, l_recv, k))
    for tile in range(1, GRAD_TILES):
        grad_tile(tile)

    for k in range(1, n):
        small_arrival(loss_out, l_send, l_recv, k).wait_recv()
    whole = loss_out[0][0:1, :]
    count = total()
    for b in range(1, n):
        whole = whole + loss_out[b][0:1, :]
    loss_ref[...] = jnp.broadcast_to(whole / (count * teacher_width), loss_ref.shape)

    for chunk in range(CHUNKS):
        piece = slice(chunk * half, (chunk + 1) * half)
        value = own[1, piece, :]
        rs_copy(0, steps_a - 1, chunk).wait_recv()
        value = value + got_a[steps_a - 1, piece, :].astype(F32)
        if steps_b > 0:
            rs_copy(1, steps_b - 1, chunk).wait_recv()
            value = value + got_b[steps_b - 1, piece, :].astype(F32)
        sg_ref[piece, :] = value.astype(BF16)
    for copy in sent:
        copy.wait_send()
    for condition, copy in sent_if:
        pl.when(condition)(copy.wait_send)


def finish_kernel(sg_ref, pg_ref, loss_ref, sg_hbm, pg_hbm, loss_out, sg_sem, pg_sem):
    size = pg_ref.shape[0] // GRAD_TILES
    copies = [pltpu.make_async_copy(sg_ref, sg_hbm, sg_sem)]
    for tile in range(GRAD_TILES):
        piece = pl.ds(tile * size, size)
        copies.append(pltpu.make_async_copy(pg_ref.at[piece], pg_hbm.at[piece], pg_sem.at[tile]))
    for copy in copies:
        copy.start()
    loss_out[0] = loss_ref[0, 0]
    for copy in copies:
        copy.wait()


def finish(student_grad, projector_grad, loss):
    vmem = pl.BlockSpec(memory_space=pltpu.VMEM)
    anywhere = pl.BlockSpec(memory_space=pl.ANY)
    kept = [pltpu.with_memory_space_constraint(x, pltpu.VMEM) for x in (student_grad, projector_grad, loss)]
    return pl.pallas_call(
        finish_kernel,
        out_shape=(
            jax.ShapeDtypeStruct(student_grad.shape, BF16),
            jax.ShapeDtypeStruct(projector_grad.shape, BF16),
            jax.ShapeDtypeStruct((1,), F32),
        ),
        in_specs=[vmem, vmem, vmem],
        out_specs=(anywhere, anywhere, pl.BlockSpec(memory_space=pltpu.SMEM)),
        scratch_shapes=[pltpu.SemaphoreType.DMA, pltpu.SemaphoreType.DMA((GRAD_TILES,))],
        compiler_params=pltpu.CompilerParams(vmem_limit_bytes=8 * 1024 * 1024),
    )(*kept)


def per_device(student_states, teacher_states, projector, layer_map, boundaries, valid_counts):
    n = lax.axis_size("dp")
    rows, ds_width = student_states.shape[1:]
    width = projector.shape[2]
    direct = lax.axis_size("section") == 4
    teacher = teacher_states if direct else relayed(teacher_states, layer_map, boundaries)[None]
    steps_a, steps_b = n // 2, n - 1 - n // 2
    smem = pl.BlockSpec(memory_space=pltpu.SMEM)
    vmem = pl.BlockSpec(memory_space=pltpu.VMEM)
    anywhere = pl.BlockSpec(memory_space=pl.ANY)
    dma = pltpu.SemaphoreType.DMA
    student_grad, projector_grad, loss = pl.pallas_call(
        functools.partial(main_kernel, n, direct),
        out_shape=(
            pltpu.VMEM((rows, ds_width), BF16),
            pltpu.VMEM((ds_width, width), BF16),
            pltpu.VMEM((8, 128), F32),
        ),
        in_specs=[smem, smem, smem, anywhere, anywhere, anywhere],
        out_specs=(vmem, vmem, vmem),
        scratch_shapes=[
            pltpu.VMEM(teacher.shape, BF16),
            pltpu.VMEM((8, 128), F32),
            pltpu.VMEM((ds_width, width), BF16),
            pltpu.VMEM((n * rows, ds_width), BF16),
            pltpu.VMEM((n, rows, width), BF16),
            pltpu.VMEM((n * rows, width), BF16),
            pltpu.VMEM((n * rows, width), F32),
            pltpu.VMEM((n * rows, width), BF16),
            pltpu.VMEM((2, rows, ds_width), F32),
            pltpu.VMEM((steps_a, rows, ds_width), BF16),
            pltpu.VMEM((max(steps_b, 1), rows, ds_width), BF16),
            pltpu.VMEM((steps_a, rows, ds_width), BF16),
            pltpu.VMEM((max(steps_b, 1), rows, ds_width), BF16),
            pltpu.VMEM((n, 8, 128), F32),
            pltpu.VMEM((n, 8, width), F32),
            pltpu.VMEM((n, 8, 128), F32),
            dma,
            dma((teacher.shape[0],)),
            dma,
            dma((3, n, CHUNKS)),
            dma((n, CHUNKS)),
            dma((n, n)),
            dma((n,)),
            dma((2, steps_a, CHUNKS)),
            dma((2, steps_a, CHUNKS)),
            dma((n,)),
            dma((n,)),
            dma((n,)),
            dma((n,)),
            pltpu.VMEM((n // 2, rows, width), BF16),
            dma((n // 2,)),
            dma((n // 2,)),
            pltpu.SemaphoreType.REGULAR((n // 2 - 1,)),
        ],
        compiler_params=pltpu.CompilerParams(
            collective_id=0, has_side_effects=True, vmem_limit_bytes=56 * 1024 * 1024
        ),
    )(layer_map, boundaries, valid_counts, student_states[0], teacher, projector[0])
    student_grad, projector_grad, loss = finish(student_grad, projector_grad, loss)
    return student_grad[None], projector_grad[None], loss


def solution(mesh):
    in_specs = (
        P("section", "dp", None),
        P("section", "dp", None),
        P("section", None, "dp"),
        P(),
        P(),
        P("dp"),
    )
    out_specs = (P("section", "dp", None), P("section", None, "dp"), P("section"))
    return jax.shard_map(
        per_device, mesh=mesh, in_specs=in_specs, out_specs=out_specs, check_vma=False
    )
```

```python
import functools

import jax
import jax.numpy as jnp
from jax import lax
from jax.experimental import pallas as pl
from jax.experimental.pallas import tpu as pltpu
from jax.sharding import PartitionSpec as P

loss_scale = 128.0
norm_eps = 1e-06
MESH = pl.DeviceIdType.MESH
F32, BF16 = jnp.float32, jnp.bfloat16
CHUNKS = 4
GRAD_TILES = 8


def from_behind(block, axis, distance):
    devices = range(lax.axis_size(axis))
    route = [(i - distance, i) for i in devices if i - distance in devices]
    return lax.ppermute(block, axis, route)


def lookup(table, index):
    places = jnp.arange(table.shape[0], dtype=jnp.int32)
    return jnp.sum(jnp.where(places == index, table, 0))


def relayed(teacher_states, layer_map, boundaries):
    sections = lax.axis_size("section")
    here = lax.axis_index("section")
    held_slots = teacher_states.shape[0]
    inner = boundaries[1:sections]
    owners = jnp.sum((inner[None, :] <= layer_map[:, None]).astype(jnp.int32), axis=1)
    first_layer = lookup(boundaries, here)

    def outgoing(offset):
        destination = here + offset
        inside = (destination >= 0) & (destination < sections)
        wanted = lookup(layer_map, destination)
        owner = lookup(owners, destination)
        place = jnp.clip(wanted - first_layer, 0, held_slots - 1)
        piece = lax.dynamic_index_in_dim(teacher_states, place, 0, keepdims=False)
        return jnp.where(inside & (owner == here), piece, jnp.zeros_like(piece))

    needed = here - lookup(owners, here)
    arrivals = []
    for offset in (-1, 1):
        stacked = jnp.stack([outgoing(offset), outgoing(2 * offset)])
        first_arrived = from_behind(stacked, "section", offset)
        second_arrived = from_behind(first_arrived[1:2], "section", offset)
        arrivals.append((offset, first_arrived[0]))
        arrivals.append((2 * offset, second_arrived[0]))
    hidden = outgoing(0)
    for offset, arrived in arrivals:
        hidden = jnp.where(needed == offset, arrived, hidden)
    return hidden


def send_to(here):
    return 2 - 2 * here + 5 * (here // 2)


def taken_from(here):
    return 1 + 2 * here - 5 * (here // 2)


def arrival_order(place, lines):
    order = []
    for step in range(lines - 1):
        sides = (place - 1 - step, place + 1 + step)
        order += [b for b in (sides if 2 * place < lines else sides[::-1]) if 0 <= b < lines]
    return order


def ring_start(n, steps_a, steps_b):
    lines = n // 2
    ring = [2 * p for p in range(lines)] + [2 * (n - 1 - p) + 1 for p in range(lines, n)]
    for step in range(1, lines - 1):
        ready = True
        for place in range(n):
            line, pair = ring[place] // 2, ring[place] % 2
            late = [b for k, b in enumerate(arrival_order(line, lines)) if k == 0 or k > step]
            late = [2 * b + 1 - pair for b in late]
            needed = [ring[(place + sign * offset) % n] for sign in (1, -1) for offset in (steps_a, -steps_b)]
            ready = ready and not set(late) & set(needed)
        if ready:
            return step
    return lines - 1


def main_kernel(n, direct, map_ref, bounds_ref, counts_ref, s_hbm, t_hbm, w_hbm, sg_ref, pg, loss_ref,
                teacher, count_ref, weights, stud, normed, tgt, proj, scaled, own, part_a, part_b, got_a, got_b,
                counts, losses, loss_out,
                in_sem, slab_sem, w_sem, ag_send, ag_recv, t_send, t_recv, rs_send, rs_recv,
                c_send, c_recv, l_send, l_recv, passing, p_send, p_recv, rounds):
    here = lax.axis_index("section")
    me = lax.axis_index("dp")
    rows, ds_width = s_hbm.shape
    width = weights.shape[1]
    half = rows // CHUNKS
    steps_a, steps_b = n // 2, n - 1 - n // 2
    teacher_width = width * n

    pair, line = me % 2, me // 2
    partner = me + 1 - 2 * pair
    lines = n // 2
    can_up, can_down = line < lines - 1, line > 0
    x, z = me % 2, me // 2
    position = z * (1 - x) + (n - 1 - z) * x
    sign = 1 - 2 * (here % 2)

    def at(offset):
        p = (position + sign * offset + 2 * n) % n
        low = 1 - p // (n // 2)
        return low * (2 * p) + (1 - low) * (2 * (n - 1 - p) + 1)

    after, before = at(1), at(-1)

    def block(index):
        return pl.ds(pl.multiple_of(index * rows, rows), rows)

    load_students = pltpu.make_async_copy(s_hbm, stud.at[block(me)], in_sem)
    load_students.start()
    held = teacher.shape[0]
    load_teacher = [
        pltpu.make_async_copy(t_hbm.at[slot], teacher.at[slot], slab_sem.at[slot]) for slot in range(held)
    ]
    barrier = pltpu.get_barrier_semaphore()
    near = 2 - line // (lines - 1) + (line + lines - 1) // lines + 2 * direct

    def greet(semaphore):
        def signal(section, device):
            pl.semaphore_signal(semaphore, inc=1, device_id=(section, device), device_id_type=MESH)

        signal(here, partner)
        pl.when(can_up)(lambda: signal(here, me + 2))
        pl.when(can_down)(lambda: signal(here, me - 2))
        if direct:
            signal(send_to(here), me)
            signal(taken_from(here), me)

    def next_round(k):
        if k > 0:
            pl.semaphore_wait(rounds.at[k - 1], near)
        if k < lines - 1:
            greet(rounds.at[k])

    load_weights = pltpu.make_async_copy(w_hbm, weights, w_sem)
    greet(barrier)
    for copy in load_teacher:
        copy.start()
    load_weights.start()
    count_ref[...] = jnp.full(count_ref.shape, counts_ref[0].astype(F32), F32)
    pl.semaphore_wait(barrier, near)
    load_students.wait()


    def reached(place):
        return (line + lines - place) // lines

    def arrival_of(k):
        value = 0
        for place in range(lines):
            value = value + arrival_order(place, lines)[k] * (reached(place) - reached(place + 1))
        return value

    def piece_of(index, chunk):
        return stud.at[pl.ds(pl.multiple_of(index * rows + chunk * half, half), half)]

    UP, DOWN, ACROSS = 0, 1, 2
    targets_of = (me + 2, me - 2, me + 1 - 2 * pair)

    def ag_copy(way, index, step, chunk):
        return pltpu.make_async_remote_copy(
            src_ref=piece_of(index, chunk), dst_ref=piece_of(index, chunk),
            send_sem=ag_send.at[way, step, chunk], recv_sem=ag_recv.at[index, chunk],
            device_id=(here, targets_of[way]), device_id_type=MESH)

    def ag_arrival(index, chunk):
        return pltpu.make_async_remote_copy(
            src_ref=piece_of(index, chunk), dst_ref=piece_of(index, chunk),
            send_sem=ag_send.at[0, 0, chunk], recv_sem=ag_recv.at[index, chunk],
            device_id=(here, targets_of[2]), device_id_type=MESH)

    ag_steps = (steps_a, steps_b)
    sent = []
    sent_if = []

    def go(copy):
        copy.start()
        sent.append(copy)

    def go_if(condition, copy):
        pl.when(condition)(copy.start)
        sent_if.append((condition, copy))

    for chunk in range(CHUNKS):
        go_if(can_up, ag_copy(UP, me, 0, chunk))
        go_if(can_down, ag_copy(DOWN, me, 0, chunk))
        go(ag_copy(ACROSS, me, 0, chunk))

    def relay(step):
        below, above = me - 2 - 2 * step, me + 2 + 2 * step
        from_below, from_above = line - 1 - step >= 0, line + 1 + step < lines
        for chunk in range(CHUNKS):
            pl.when(from_below)(ag_arrival(below, chunk).wait_recv)
            go_if(from_below & can_up, ag_copy(UP, below, step + 1, chunk))
            pl.when(from_above)(ag_arrival(above, chunk).wait_recv)
            go_if(from_above & can_down, ag_copy(DOWN, above, step + 1, chunk))

    def relay_across(k):
        for chunk in range(CHUNKS):
            go(ag_copy(ACROSS, 2 * arrival_of(k) + pair, k + 1, chunk))

    def other_line(m):
        value, bit = 0, 1
        while bit < lines:
            mine = (line // bit) % 2
            flip = (m // bit) % 2
            value = value + bit * (mine + flip - 2 * mine * flip)
            bit *= 2
        return value

    def small(source, slots, send_sems, recv_sems, k):
        peer = (me + k) % n
        return pltpu.make_async_remote_copy(
            src_ref=source, dst_ref=slots.at[me], send_sem=send_sems.at[k], recv_sem=recv_sems.at[me],
            device_id=(here, peer), device_id_type=MESH)

    def small_arrival(slots, send_sems, recv_sems, k):
        peer = (me + k) % n
        return pltpu.make_async_remote_copy(
            src_ref=slots.at[peer], dst_ref=slots.at[peer], send_sem=send_sems.at[k],
            recv_sem=recv_sems.at[peer], device_id=(here, peer), device_id_type=MESH)

    counts[me] = count_ref[...]
    next_round(0)

    for copy in load_teacher:
        copy.wait()
    place = 0
    if direct:
        place = jnp.clip(map_ref[send_to(here)] - bounds_ref[here], 0, held - 1)
    squares = jnp.zeros((rows, 1), F32)
    for g in range(n):
        h = teacher[place, :, g * width:(g + 1) * width].astype(F32)
        squares += jnp.sum(h * h, axis=1, keepdims=True)
    next_round(1)
    inverse = lax.rsqrt(squares / teacher_width + norm_eps)
    for g in range(n):
        h = teacher[place, :, g * width:(g + 1) * width].astype(F32)
        normed[g] = (h * inverse).astype(BF16)
    taker = send_to(here) if direct else here

    def target_copy(source, owner, g):
        return pltpu.make_async_remote_copy(
            src_ref=source, dst_ref=tgt.at[block(owner)], send_sem=t_send.at[owner, g], recv_sem=t_recv.at[owner],
            device_id=(taker, g), device_id_type=MESH)

    def crossing(k):
        g = 2 * other_line(k) + 1 - pair
        return pltpu.make_async_remote_copy(
            src_ref=normed.at[g], dst_ref=passing.at[k], send_sem=p_send.at[k], recv_sem=p_recv.at[k],
            device_id=(here, partner), device_id_type=MESH)

    def own_target(k):
        g = 2 * other_line(k) + pair
        return target_copy(normed.at[g], me, g)

    def passed_target(k):
        g = 2 * other_line(k) + pair
        return target_copy(passing.at[k], partner, g)

    def target_arrival(index):
        return pltpu.make_async_remote_copy(
            src_ref=tgt.at[block(index)], dst_ref=tgt.at[block(index)], send_sem=t_send.at[0, index],
            recv_sem=t_recv.at[index], device_id=(taker, index), device_id_type=MESH)

    if not direct:
        tgt[block(me), :] = normed[me]
    far_first = range(lines - 1, 0, -1)
    for k in far_first:
        go(crossing(k))
    for k in range(2, lines):
        next_round(k)
    go(target_copy(normed.at[partner], me, partner))
    if direct:
        go(own_target(0))

    def project(index):
        proj[block(index), :] = jnp.dot(stud[block(index), :], weights[...], preferred_element_type=F32)

    row = lax.broadcasted_iota(jnp.int32, (rows, 1), 0).astype(F32)
    losses[me] = jnp.zeros(losses.shape[1:], F32)

    def total():
        value = counts[0][0:1, :]
        for b in range(1, n):
            value = value + counts[b][0:1, :]
        return value

    def residual(offset):
        index = at(offset)
        if direct or offset != 0:
            target_arrival(index).wait_recv()
        left = proj[block(index), :] - tgt[block(index), :].astype(F32)
        valid = jnp.where(row < counts[index][0:1, 0:1], 1.0, 0.0)
        kept = valid * left
        line = jnp.sum(kept * left, axis=0, keepdims=True)
        losses[me] += jnp.broadcast_to(line, losses.shape[1:])
        scaled[block(index), :] = (loss_scale / total()[:, 0:1] * kept).astype(BF16)

    def share(offset, into):
        own[into] = lax.dot_general(
            scaled[block(at(offset)), :], weights[...], (((1,), (1,)), ((), ())), preferred_element_type=F32)

    def rs_copy(direction, step, chunk):
        parts, gots = (part_a, got_a) if direction == 0 else (part_b, got_b)
        piece = pl.ds(chunk * half, half)
        return pltpu.make_async_remote_copy(
            src_ref=parts.at[step, piece], dst_ref=gots.at[step, piece],
            send_sem=rs_send.at[direction, step, chunk], recv_sem=rs_recv.at[direction, step, chunk],
            device_id=(here, after if direction == 0 else before), device_id_type=MESH)

    def grad_tile(tile):
        size = ds_width // GRAD_TILES
        left = stud[:, tile * size:(tile + 1) * size]
        pg[tile * size:(tile + 1) * size, :] = lax.dot_general(
            left, scaled[...], (((0,), (0,)), ((), ())), preferred_element_type=F32).astype(BF16)

    def advance(step, directions):
        for chunk in range(CHUNKS):
            piece = slice(chunk * half, (chunk + 1) * half)
            for direction in directions:
                if step >= ag_steps[direction]:
                    continue
                parts, gots = (part_a, got_a) if direction == 0 else (part_b, got_b)
                value = own[direction, piece, :]
                if step > 0:
                    rs_copy(direction, step - 1, chunk).wait_recv()
                    value = value + gots[step - 1, piece, :].astype(F32)
                parts[step, piece, :] = value.astype(BF16)
                go(rs_copy(direction, step, chunk))

    def prepare(step, direction):
        if step < ag_steps[direction]:
            offset = steps_a - step if direction == 0 else step - steps_b
            residual(offset)
            share(offset, direction)

    def project_across(source):
        index = 2 * source + 1 - pair
        for chunk in range(CHUNKS):
            ag_arrival(index, chunk).wait_recv()
        project(index)

    load_weights.wait()
    project(me)
    middle = min(1, lines - 2)
    for step in range(lines - 1):
        relay(step)
        if step == 0:
            for k in range(1, n):
                go(small(count_ref, counts, c_send, c_recv, k))
        if step == middle:
            for k in far_first:
                go(own_target(k))
        if step > 0:
            relay_across(step)
        if step == lines - 2:
            relay_across(0)
        project(2 * arrival_of(step) + pair)
        if step == 0:
            project_across(line)
        if step == middle:
            for k in far_first:
                crossing(k).wait_recv()
                go(passed_target(k))
    start = ring_start(n, steps_a, steps_b)
    for k in range(1, n):
        small_arrival(counts, c_send, c_recv, k).wait_recv()
    for step in range(1, lines):
        project_across(arrival_of(step % (lines - 1)))
        if step == start:
            prepare(0, 0)
            advance(0, (0,))
            prepare(0, 1)
            advance(0, (1,))

    for step in range(1, steps_a):
        prepare(step, 1)
        prepare(step, 0)
        if step == steps_a - 1:
            residual(0)
            share(0, 1)
        advance(step, (1, 0))

    line = losses[me][0:1, :]
    folded = jnp.sum(line, axis=1, keepdims=True)
    loss_out[me] = jnp.broadcast_to(folded, loss_out.shape[1:])
    grad_tile(0)
    for k in range(1, n):
        go(small(loss_out.at[me], loss_out, l_send, l_recv, k))
    for tile in range(1, GRAD_TILES):
        grad_tile(tile)

    for k in range(1, n):
        small_arrival(loss_out, l_send, l_recv, k).wait_recv()
    whole = loss_out[0][0:1, :]
    count = total()
    for b in range(1, n):
        whole = whole + loss_out[b][0:1, :]
    loss_ref[...] = jnp.broadcast_to(whole / (count * teacher_width), loss_ref.shape)

    for chunk in range(CHUNKS):
        piece = slice(chunk * half, (chunk + 1) * half)
        value = own[1, piece, :]
        rs_copy(0, steps_a - 1, chunk).wait_recv()
        value = value + got_a[steps_a - 1, piece, :].astype(F32)
        if steps_b > 0:
            rs_copy(1, steps_b - 1, chunk).wait_recv()
            value = value + got_b[steps_b - 1, piece, :].astype(F32)
        sg_ref[piece, :] = value.astype(BF16)
    for copy in sent:
        copy.wait_send()
    for condition, copy in sent_if:
        pl.when(condition)(copy.wait_send)


def finish_kernel(sg_ref, pg_ref, loss_ref, sg_hbm, pg_hbm, loss_out, sg_sem, pg_sem):
    size = pg_ref.shape[0] // GRAD_TILES
    copies = [pltpu.make_async_copy(sg_ref, sg_hbm, sg_sem)]
    for tile in range(GRAD_TILES):
        piece = pl.ds(tile * size, size)
        copies.append(pltpu.make_async_copy(pg_ref.at[piece], pg_hbm.at[piece], pg_sem.at[tile]))
    for copy in copies:
        copy.start()
    loss_out[0] = loss_ref[0, 0]
    for copy in copies:
        copy.wait()


def finish(student_grad, projector_grad, loss):
    vmem = pl.BlockSpec(memory_space=pltpu.VMEM)
    anywhere = pl.BlockSpec(memory_space=pl.ANY)
    kept = [pltpu.with_memory_space_constraint(x, pltpu.VMEM) for x in (student_grad, projector_grad, loss)]
    return pl.pallas_call(
        finish_kernel,
        out_shape=(
            jax.ShapeDtypeStruct(student_grad.shape, BF16),
            jax.ShapeDtypeStruct(projector_grad.shape, BF16),
            jax.ShapeDtypeStruct((1,), F32),
        ),
        in_specs=[vmem, vmem, vmem],
        out_specs=(anywhere, anywhere, pl.BlockSpec(memory_space=pltpu.SMEM)),
        scratch_shapes=[pltpu.SemaphoreType.DMA, pltpu.SemaphoreType.DMA((GRAD_TILES,))],
        compiler_params=pltpu.CompilerParams(vmem_limit_bytes=8 * 1024 * 1024),
    )(*kept)


def per_device(student_states, teacher_states, projector, layer_map, boundaries, valid_counts):
    n = lax.axis_size("dp")
    rows, ds_width = student_states.shape[1:]
    width = projector.shape[2]
    direct = lax.axis_size("section") == 4
    teacher = teacher_states if direct else relayed(teacher_states, layer_map, boundaries)[None]
    steps_a, steps_b = n // 2, n - 1 - n // 2
    smem = pl.BlockSpec(memory_space=pltpu.SMEM)
    vmem = pl.BlockSpec(memory_space=pltpu.VMEM)
    anywhere = pl.BlockSpec(memory_space=pl.ANY)
    dma = pltpu.SemaphoreType.DMA
    student_grad, projector_grad, loss = pl.pallas_call(
        functools.partial(main_kernel, n, direct),
        out_shape=(
            pltpu.VMEM((rows, ds_width), BF16),
            pltpu.VMEM((ds_width, width), BF16),
            pltpu.VMEM((8, 128), F32),
        ),
        in_specs=[smem, smem, smem, anywhere, anywhere, anywhere],
        out_specs=(vmem, vmem, vmem),
        scratch_shapes=[
            pltpu.VMEM(teacher.shape, BF16),
            pltpu.VMEM((8, 128), F32),
            pltpu.VMEM((ds_width, width), BF16),
            pltpu.VMEM((n * rows, ds_width), BF16),
            pltpu.VMEM((n, rows, width), BF16),
            pltpu.VMEM((n * rows, width), BF16),
            pltpu.VMEM((n * rows, width), F32),
            pltpu.VMEM((n * rows, width), BF16),
            pltpu.VMEM((2, rows, ds_width), F32),
            pltpu.VMEM((steps_a, rows, ds_width), BF16),
            pltpu.VMEM((max(steps_b, 1), rows, ds_width), BF16),
            pltpu.VMEM((steps_a, rows, ds_width), BF16),
            pltpu.VMEM((max(steps_b, 1), rows, ds_width), BF16),
            pltpu.VMEM((n, 8, 128), F32),
            pltpu.VMEM((n, 8, width), F32),
            pltpu.VMEM((n, 8, 128), F32),
            dma,
            dma((teacher.shape[0],)),
            dma,
            dma((3, n, CHUNKS)),
            dma((n, CHUNKS)),
            dma((n, n)),
            dma((n,)),
            dma((2, steps_a, CHUNKS)),
            dma((2, steps_a, CHUNKS)),
            dma((n,)),
            dma((n,)),
            dma((n,)),
            dma((n,)),
            pltpu.VMEM((n // 2, rows, width), BF16),
            dma((n // 2,)),
            dma((n // 2,)),
            pltpu.SemaphoreType.REGULAR((n // 2 - 1,)),
        ],
        compiler_params=pltpu.CompilerParams(
            collective_id=0, has_side_effects=True, vmem_limit_bytes=56 * 1024 * 1024
        ),
    )(layer_map, boundaries, valid_counts, student_states[0], teacher, projector[0])
    student_grad, projector_grad, loss = finish(student_grad, projector_grad, loss)
    return student_grad[None], projector_grad[None], loss


def solution(mesh):
    in_specs = (
        P("section", "dp", None),
        P("section", "dp", None),
        P("section", None, "dp"),
        P(),
        P(),
        P("dp"),
    )
    out_specs = (P("section", "dp", None), P("section", None, "dp"), P("section"))
    return jax.shard_map(
        per_device, mesh=mesh, in_specs=in_specs, out_specs=out_specs, check_vma=False
    )
```
